8 devices in a mesh: dp: 1 (over z), ep2: 2 (over y), ep: 4 (over x, core).
Axes of the slice: x: 2, y: 2, z: 1, core: 2. Of those that a mesh axis runs over, the one named last changes fastest.
Arguments:
- tokens: bfloat16 [1024, 1536], P(('dp', 'ep2', 'ep'))
- expert_idx: int32 [1024, 8], P(('dp', 'ep2', 'ep'))
- gates: float32 [1024, 8], P(('dp', 'ep2', 'ep'))
- w_gate: bfloat16 [40, 1536, 512], P(('ep2', 'ep'))
- w_up: bfloat16 [40, 1536, 512], P(('ep2', 'ep'))
- w_down: bfloat16 [40, 512, 1536], P(('ep2', 'ep'))
Outputs:
- output: bfloat16 [1024, 1536], P(('dp', 'ep2', 'ep'))
All inputs are finite; a program needn't handle non-finite values.
Results may differ from the reference program's by a relative error of at most 0.001.
Values are sent between devices in bfloat16 or wider.
A program may use at most 1 GiB of HBM per device.

```python
import jax
import jax.numpy as jnp
from jax import lax

GROUP_DEVS = 8
TOKENS = 128
HIDDEN = 1536
EXPERT_FF = 512
EXPERTS = 40
TOP_K = 8

LOCAL_EXPERTS = EXPERTS // GROUP_DEVS
EXPERT_CAP = (TOKENS * TOP_K + EXPERTS - 1) // EXPERTS
TOTAL_ROWS = GROUP_DEVS * TOKENS
EXPERT_ROWS = GROUP_DEVS * EXPERT_CAP


def draw_routing(route_key):
    key_pick, key_first, key_rest, key_bias = jax.random.split(route_key, 4)
    expert_ids = jnp.arange(EXPERTS, dtype=jnp.int32)
    local_pick = jax.random.randint(key_pick, (GROUP_DEVS, GROUP_DEVS), 0, LOCAL_EXPERTS)
    picked = (expert_ids % LOCAL_EXPERTS)[None, :] == jnp.repeat(local_pick, LOCAL_EXPERTS, axis=1)
    first_score = jax.random.randint(key_first, (GROUP_DEVS, EXPERTS), 0, 1024) + 2048
    rest_score = jax.random.randint(key_rest, (GROUP_DEVS, EXPERTS), 0, 1024) + jax.random.randint(key_bias, (1, EXPERTS), 0, 512)
    score = jnp.where(picked, first_score, rest_score) * EXPERTS + expert_ids[None, :]
    sequence = jnp.argsort(-score, axis=1).astype(jnp.int32)
    positions = (jnp.arange(TOKENS)[:, None] * TOP_K + jnp.arange(TOP_K)[None, :]) % EXPERTS
    chosen = jnp.take(sequence, positions.reshape(-1), axis=1)
    return chosen.reshape(TOTAL_ROWS, TOP_K)


def setup_inputs(seed: int = 0, part: int = 0) -> dict:
    root_key = jax.random.key(seed)
    shared_key, local_root = jax.random.split(root_key)
    part_key = jax.random.fold_in(local_root, part)
    key_tok, key_route, key_gate = jax.random.split(part_key, 3)
    key_wg, key_wu, key_wd = jax.random.split(shared_key, 3)
    tokens = jax.random.normal(key_tok, (TOTAL_ROWS, HIDDEN), jnp.float32).astype(jnp.bfloat16)
    expert_idx = draw_routing(key_route)
    gate_logits = jax.random.normal(key_gate, (TOTAL_ROWS, TOP_K), jnp.float32)
    gates = 0.5 * TOP_K * jax.nn.softmax(gate_logits, axis=-1)
    w_gate = (jax.random.normal(key_wg, (EXPERTS, HIDDEN, EXPERT_FF), jnp.float32) * HIDDEN ** -0.5).astype(jnp.bfloat16)
    w_up = (jax.random.normal(key_wu, (EXPERTS, HIDDEN, EXPERT_FF), jnp.float32) * HIDDEN ** -0.5).astype(jnp.bfloat16)
    w_down = (jax.random.normal(key_wd, (EXPERTS, EXPERT_FF, HIDDEN), jnp.float32) * EXPERT_FF ** -0.5).astype(jnp.bfloat16)
    return {'tokens': tokens, 'expert_idx': expert_idx, 'gates': gates, 'w_gate': w_gate, 'w_up': w_up, 'w_down': w_down}


def expert_ffn(operands):
    rows_in, gate_w, up_w, down_w = operands
    act_gate = jnp.dot(rows_in, gate_w, preferred_element_type=jnp.float32)
    act_up = jnp.dot(rows_in, up_w, preferred_element_type=jnp.float32)
    inner_act = (jax.nn.silu(act_gate) * act_up).astype(jnp.bfloat16)
    return jnp.dot(inner_act, down_w, preferred_element_type=jnp.float32).astype(jnp.bfloat16)


def reference(tokens, expert_idx, gates, w_gate, w_up, w_down):
    flat_ids = expert_idx.reshape(-1)
    n_items = flat_ids.shape[0]
    sort_order = jnp.argsort(flat_ids, stable=True)
    sorted_ids = flat_ids[sort_order]
    counts = jnp.bincount(flat_ids, length=EXPERTS)
    starts = jnp.cumsum(counts) - counts
    rank_sorted = (jnp.arange(n_items) - starts[sorted_ids]).astype(jnp.int32)
    slot_rank = jnp.zeros((n_items,), jnp.int32).at[sort_order].set(rank_sorted)
    token_of = jnp.arange(n_items) // TOP_K
    expert_in = jnp.zeros((EXPERTS, EXPERT_ROWS, HIDDEN), tokens.dtype).at[flat_ids, slot_rank].set(tokens[token_of])
    expert_out = lax.map(expert_ffn, (expert_in, w_gate, w_up, w_down))
    routed = expert_out[flat_ids, slot_rank].reshape(TOTAL_ROWS, TOP_K, HIDDEN)
    mixed = jnp.sum(gates[:, :, None] * routed.astype(jnp.float32), axis=1)
    return (tokens.astype(jnp.float32) + mixed).astype(jnp.bfloat16)
```

```python
import itertools

import jax
import jax.numpy as jnp
from jax import lax
from jax.experimental import pallas as pl
from jax.experimental.pallas import tpu as pltpu
from jax.sharding import PartitionSpec as P

MESH = pl.DeviceIdType.MESH
F32 = jnp.float32
BF16 = jnp.bfloat16
OWN, XN, YN, DG = 0, 1, 2, 3
SLOT = 32
GROUPS = (((XN, 0), (XN, 1), (YN, 0), (YN, 1)), ((DG, 0), (DG, 1), (OWN, 0), (OWN, 1)))
PIECES = 3


def moe_kernel(
    tok_ref, idx_ref, gate_ref, wg_hbm, wu_hbm, wd_hbm, out_ref,
    wg, wu, wd, toks, idxs, gats, pick, mix, xg, hid, yc, ys, part, relx, rely, finx, finy,
    wsem, ssem, rsem,
):
    n_exp = wg.shape[0]
    rows, d_model = tok_ref.shape
    half = rows // 2
    width = d_model // PIECES
    n_slot = n_exp * SLOT
    top_k = idx_ref.shape[0]

    loads = {}
    wids = itertools.count()
    for name, src, dst in (("g", wg_hbm, wg), ("u", wu_hbm, wu), ("d", wd_hbm, wd)):
        for e in range(n_exp):
            loads[name, e] = pltpu.make_async_copy(src.at[e], dst.at[e], wsem.at[next(wids)])
    for e in range(n_exp):
        loads["g", e].start()
        loads["u", e].start()
    for e in range(n_exp):
        loads["d", e].start()

    iy = lax.axis_index("ep2")
    ie = lax.axis_index("ep")
    ix = ie // 2
    ic = ie % 2
    to_x = {"ep2": iy, "ep": (1 - ix) * 2 + ic}
    to_y = {"ep2": 1 - iy, "ep": ie}
    to_c = {"ep2": iy, "ep": ix * 2 + 1 - ic}
    base_own = (iy * 4 + ie) * n_exp
    base_par = (iy * 4 + ix * 2 + 1 - ic) * n_exp

    barrier = pltpu.get_barrier_semaphore()
    for peer in (to_x, to_y, to_c):
        pl.semaphore_signal(barrier, inc=1, device_id=peer, device_id_type=MESH)
    pl.semaphore_wait(barrier, 3)

    ids = itertools.count()
    sent = []

    def send(src, dst, peer):
        i = next(ids)
        copy = pltpu.make_async_remote_copy(
            src_ref=src, dst_ref=dst, send_sem=ssem.at[i], recv_sem=rsem.at[i],
            device_id=peer, device_id_type=MESH,
        )
        copy.start()
        sent.append(copy)
        return copy

    lo, hi = pl.ds(0, half), pl.ds(half, half)

    def send_route(src_i, src_g, slot, peer):
        return (send(src_i, idxs.at[slot], peer), send(src_g, gats.at[slot], peer))

    def send_rows(src, slot, part_rows, peer):
        return send(src.at[part_rows], toks.at[slot].at[part_rows], peer)

    r_x = send_route(idx_ref, gate_ref, (XN, 0), to_x)
    r_y = send_route(idx_ref, gate_ref, (YN, 0), to_y)
    r_c = send_route(idx_ref, gate_ref, (OWN, 1), to_c)
    t_x0 = send_rows(tok_ref, (XN, 0), lo, to_x)
    t_y1 = send_rows(tok_ref, (YN, 0), hi, to_y)
    t_x1 = send_rows(tok_ref, (XN, 0), hi, to_x)
    t_y0 = send_rows(tok_ref, (YN, 0), lo, to_y)
    t_c = send(tok_ref, toks.at[OWN, 1], to_c)

    def wait_all(copies):
        for copy in copies:
            copy.wait_recv()

    sub16 = lax.broadcasted_iota(jnp.int32, (16, rows), 0)
    exp_id = jnp.where(sub16 < 8, base_own + sub16, base_par + sub16 - 8)
    before = (
        lax.broadcasted_iota(jnp.int32, (rows, rows), 0)
        < lax.broadcasted_iota(jnp.int32, (rows, rows), 1)
    ).astype(F32).astype(BF16)
    place = lax.broadcasted_iota(jnp.int32, (SLOT, rows), 0).astype(F32)

    def prepare(chip, core):
        if (chip, core) == (OWN, 0):
            idx, gat = idx_ref[...], gate_ref[...]
        else:
            idx, gat = idxs[chip, core], gats[chip, core]
        chosen = jnp.zeros((16, rows), F32)
        weight = jnp.zeros((16, rows), F32)
        for j in range(top_k):
            hit = jnp.broadcast_to(idx[j:j + 1, :], (16, rows)) == exp_id
            chosen = jnp.where(hit, 1.0, chosen)
            weight = jnp.where(hit, jnp.broadcast_to(gat[j:j + 1, :], (16, rows)), weight)
        rank = jnp.dot(chosen.astype(BF16), before, preferred_element_type=F32)
        rank = jnp.where(chosen > 0.0, rank, -1.0)
        for e in range(n_exp):
            here = jnp.broadcast_to(rank[e:e + 1, :], (SLOT, rows)) == place
            pick[chip, core, pl.ds(e * SLOT, SLOT), :] = jnp.where(here, 1.0, 0.0).astype(BF16)
        if core == 0:
            cols = []
            for k in range(2 * n_exp):
                row = k if k < n_exp else 8 + k - n_exp
                here = jnp.broadcast_to(rank[row:row + 1, :], (SLOT, rows)) == place
                cols.append(jnp.where(here, jnp.broadcast_to(weight[row:row + 1, :], (SLOT, rows)), 0.0))
            full = jnp.concatenate(cols, axis=0).T
            first = full.astype(BF16)
            rest = full - first.astype(F32)
            second = rest.astype(BF16)
            mix[chip, 0] = first
            mix[chip, 1] = second
            mix[chip, 2] = (rest - second.astype(F32)).astype(BF16)

    def gather(k, chip, core):
        src = tok_ref if (chip, core) == (OWN, 0) else toks.at[chip, core]
        for n in range(PIECES):
            cols = pl.ds(n * width, width)
            got = jnp.dot(pick[chip, core], src[:, cols], preferred_element_type=F32).astype(BF16)
            for e in range(n_exp):
                xg[e, pl.ds(k * SLOT, SLOT), cols] = got[e * SLOT:(e + 1) * SLOT, :]

    def up_gate(e):
        a = jnp.dot(xg[e], wg[e], preferred_element_type=F32)
        b = jnp.dot(xg[e], wu[e], preferred_element_type=F32)
        hid[e] = (jax.nn.silu(a) * b).astype(BF16)

    def down(group, n):
        for e in range(n_exp):
            y = jnp.dot(hid[e], wd[e, :, pl.ds(n * width, width)], preferred_element_type=F32).astype(BF16)
            for k, (chip, core) in enumerate(group):
                piece = y[k * SLOT:(k + 1) * SLOT, :]
                if core == 0:
                    yc[chip, n, pl.ds(e * SLOT, SLOT), :] = piece
                else:
                    ys[chip, n, pl.ds(e * SLOT, SLOT), :] = piece
        return {
            chip: send(ys.at[chip, n], yc.at[chip, n].at[pl.ds(n_slot, n_slot)], to_c)
            for chip, core in group if core == 1
        }

    def combine(chip, n):
        y = yc[chip, n]
        total = jnp.dot(mix[chip, 2], y, preferred_element_type=F32)
        total += jnp.dot(mix[chip, 1], y, preferred_element_type=F32)
        total += jnp.dot(mix[chip, 0], y, preferred_element_type=F32)
        part[chip, n] = total

    prepare(OWN, 0)
    wait_all(r_x)
    r_xc = send_route(idxs.at[XN, 0], gats.at[XN, 0], (XN, 1), to_c)
    r_d = send_route(idxs.at[XN, 0], gats.at[XN, 0], (DG, 0), to_y)
    wait_all(r_y)
    r_yc = send_route(idxs.at[YN, 0], gats.at[YN, 0], (YN, 1), to_c)
    prepare(XN, 0)
    prepare(YN, 0)
    wait_all(r_xc)
    prepare(XN, 1)
    wait_all(r_yc)
    prepare(YN, 1)
    wait_all(r_d)
    r_dc = send_route(idxs.at[DG, 0], gats.at[DG, 0], (DG, 1), to_c)
    prepare(DG, 0)
    wait_all(r_c)
    prepare(OWN, 1)

    t_x0.wait_recv()
    t_d0 = send_rows(toks.at[XN, 0], (DG, 0), lo, to_y)
    t_xc0 = send_rows(toks.at[XN, 0], (XN, 1), lo, to_c)
    t_y1.wait_recv()
    t_d1 = send_rows(toks.at[YN, 0], (DG, 0), hi, to_x)
    t_yc1 = send_rows(toks.at[YN, 0], (YN, 1), hi, to_c)
    wait_all(r_dc)
    prepare(DG, 1)
    t_x1.wait_recv()
    t_xc1 = send_rows(toks.at[XN, 0], (XN, 1), hi, to_c)
    t_y0.wait_recv()
    t_yc0 = send_rows(toks.at[YN, 0], (YN, 1), lo, to_c)

    gather(0, XN, 0)
    gather(2, YN, 0)
    wait_all((t_xc0, t_xc1))
    gather(1, XN, 1)
    wait_all((t_yc0, t_yc1))
    gather(3, YN, 1)
    for e in range(n_exp):
        loads["g", e].wait()
        loads["u", e].wait()
        up_gate(e)
    for e in range(n_exp):
        loads["d", e].wait()

    fin = {}

    def finish_first(n, copies):
        copies[XN].wait_recv()
        combine(XN, n)
        fin["x", 0, n] = send(part.at[XN, n].at[lo], finx.at[n].at[lo], to_x)
        copies[YN].wait_recv()
        combine(YN, n)
        fin["y", 1, n] = send(part.at[YN, n].at[hi], finy.at[n].at[hi], to_y)

    held = down(GROUPS[0], 0)
    for n in range(1, PIECES):
        nxt = down(GROUPS[0], n)
        finish_first(n - 1, held)
        held = nxt
    finish_first(PIECES - 1, held)

    t_d0.wait_recv()
    t_dc0 = send_rows(toks.at[DG, 0], (DG, 1), lo, to_c)
    t_d1.wait_recv()
    t_dc1 = send_rows(toks.at[DG, 0], (DG, 1), hi, to_c)
    gather(2, OWN, 0)
    t_c.wait_recv()
    gather(3, OWN, 1)
    gather(0, DG, 0)
    wait_all((t_dc0, t_dc1))
    gather(1, DG, 1)
    for e in range(n_exp):
        up_gate(e)

    rel = {}
    own_copies = {}

    def finish_second(n, copies):
        copies[DG].wait_recv()
        combine(DG, n)
        rel["x", n] = send(part.at[DG, n].at[lo], relx.at[n], to_x)
        rel["y", n] = send(part.at[DG, n].at[hi], rely.at[n], to_y)
        own_copies[n] = copies[OWN]

    held = down(GROUPS[1], 0)
    for n in range(1, PIECES):
        nxt = down(GROUPS[1], n)
        finish_second(n - 1, held)
        held = nxt
    finish_second(PIECES - 1, held)
    for n in range(PIECES):
        own_copies[n].wait_recv()
        combine(OWN, n)
        part[OWN, n] += tok_ref[:, pl.ds(n * width, width)].astype(F32)

    for n in range(PIECES):
        rel["x", n].wait_recv()
        part[YN, n, lo] += relx[n]
        fin["y", 0, n] = send(part.at[YN, n].at[lo], finy.at[n].at[lo], to_y)
        rel["y", n].wait_recv()
        part[XN, n, hi] += rely[n]
        fin["x", 1, n] = send(part.at[XN, n].at[hi], finx.at[n].at[hi], to_x)

    for n in range(PIECES):
        for a in "xy":
            for s in (0, 1):
                fin[a, s, n].wait_recv()
        out_ref[:, pl.ds(n * width, width)] = (part[OWN, n] + finx[n] + finy[n]).astype(BF16)
    for copy in sent:
        copy.wait_send()


def solution(mesh):
    row_spec = P(('dp', 'ep2', 'ep'), None)
    weight_spec = P(('ep2', 'ep'), None, None)

    def local_step(tokens, expert_idx, gates, w_gate, w_up, w_down):
        rows, d_model = tokens.shape
        top_k = expert_idx.shape[1]
        n_exp, _, d_ff = w_gate.shape
        width = d_model // PIECES
        n_slot = n_exp * SLOT
        vmem = pl.BlockSpec(memory_space=pltpu.VMEM)
        hbm = pl.BlockSpec(memory_space=pl.ANY)
        n_sem = 64
        return pl.pallas_call(
            moe_kernel,
            out_shape=jax.ShapeDtypeStruct((rows, d_model), BF16),
            in_specs=[vmem, vmem, vmem, hbm, hbm, hbm],
            out_specs=vmem,
            scratch_shapes=[
                pltpu.VMEM((n_exp, d_model, d_ff), BF16),
                pltpu.VMEM((n_exp, d_model, d_ff), BF16),
                pltpu.VMEM((n_exp, d_ff, d_model), BF16),
                pltpu.VMEM((4, 2, rows, d_model), BF16),
                pltpu.VMEM((4, 2, top_k, rows), jnp.int32),
                pltpu.VMEM((4, 2, top_k, rows), F32),
                pltpu.VMEM((4, 2, n_slot, rows), BF16),
                pltpu.VMEM((4, 3, rows, 2 * n_slot), BF16),
                pltpu.VMEM((n_exp, 4 * SLOT, d_model), BF16),
                pltpu.VMEM((n_exp, 4 * SLOT, d_ff), BF16),
                pltpu.VMEM((4, PIECES, 2 * n_slot, width), BF16),
                pltpu.VMEM((4, PIECES, n_slot, width), BF16),
                pltpu.VMEM((4, PIECES, rows, width), F32),
                pltpu.VMEM((PIECES, rows // 2, width), F32),
                pltpu.VMEM((PIECES, rows // 2, width), F32),
                pltpu.VMEM((PIECES, rows, width), F32),
                pltpu.VMEM((PIECES, rows, width), F32),
                pltpu.SemaphoreType.DMA((3 * n_exp,)),
                pltpu.SemaphoreType.DMA((n_sem,)),
                pltpu.SemaphoreType.DMA((n_sem,)),
            ],
            compiler_params=pltpu.CompilerParams(
                collective_id=0, has_side_effects=True, vmem_limit_bytes=62 * 1024 * 1024
            ),
            name="moe",
        )(tokens, expert_idx.T, gates.T, w_gate, w_up, w_down)

    return jax.shard_map(
        local_step, mesh=mesh,
        in_specs=(row_spec, row_spec, row_spec, weight_spec, weight_spec, weight_spec),
        out_specs=row_spec, check_vma=False,
    )
```

```python
import itertools

import jax
import jax.numpy as jnp
from jax import lax
from jax.experimental import pallas as pl
from jax.experimental.pallas import tpu as pltpu
from jax.sharding import PartitionSpec as P

MESH = pl.DeviceIdType.MESH
F32 = jnp.float32
BF16 = jnp.bfloat16
OWN, XN, YN, DG = 0, 1, 2, 3
SLOT = 32
FIRST = ((XN, 0, 0), (XN, 1, 0), (YN, 0, 1), (YN, 1, 1))
SECOND = ((DG, 0, 0), (DG, 1, 0), (DG, 0, 1), (DG, 1, 1))
THIRD = ((XN, 0, 1), (XN, 1, 1), (YN, 0, 0), (YN, 1, 0))
LAST = ((OWN, 0, 0), (OWN, 1, 0), (OWN, 0, 1), (OWN, 1, 1))
PIECES = 3


def moe_kernel(
    tok_hbm, idx_hbm, gate_hbm, wg_hbm, wu_hbm, wd_hbm, out_ref,
    wg, wu, wd, toks, idxs, gats, pick, mix, xg, hid, yc, ys, part, relx, rely, finx, finy,
    isem, wsem, ssem, rsem,
):
    n_exp = wg.shape[0]
    rows, d_model = out_ref.shape
    half = rows // 2
    width = d_model // PIECES
    n_slot = n_exp * SLOT
    top_k = idx_hbm.shape[0]

    own = [
        pltpu.make_async_copy(idx_hbm, idxs.at[OWN, 0], isem.at[0]),
        pltpu.make_async_copy(gate_hbm, gats.at[OWN, 0], isem.at[1]),
        pltpu.make_async_copy(tok_hbm, toks.at[OWN, 0], isem.at[2]),
    ]
    for copy in own:
        copy.start()

    loads = {}
    wids = itertools.count()
    for name, src, dst in (("g", wg_hbm, wg), ("u", wu_hbm, wu), ("d", wd_hbm, wd)):
        for e in range(n_exp):
            loads[name, e] = pltpu.make_async_copy(src.at[e], dst.at[e], wsem.at[next(wids)])

    iy = lax.axis_index("ep2")
    ie = lax.axis_index("ep")
    ix = ie // 2
    ic = ie % 2
    to_x = {"ep2": iy, "ep": (1 - ix) * 2 + ic}
    to_y = {"ep2": 1 - iy, "ep": ie}
    to_c = {"ep2": iy, "ep": ix * 2 + 1 - ic}
    base_own = (iy * 4 + ie) * n_exp
    base_par = (iy * 4 + ix * 2 + 1 - ic) * n_exp

    barrier = pltpu.get_barrier_semaphore()
    for peer in (to_x, to_y, to_c):
        pl.semaphore_signal(barrier, inc=1, device_id=peer, device_id_type=MESH)
    for e in range(n_exp):
        loads["g", e].start()
        loads["u", e].start()
    for e in range(n_exp):
        loads["d", e].start()
    for copy in own:
        copy.wait()
    pl.semaphore_wait(barrier, 3)

    ids = itertools.count()
    sent = []

    def send(src, dst, peer):
        i = next(ids)
        copy = pltpu.make_async_remote_copy(
            src_ref=src, dst_ref=dst, send_sem=ssem.at[i], recv_sem=rsem.at[i],
            device_id=peer, device_id_type=MESH,
        )
        copy.start()
        sent.append(copy)
        return copy

    halves = (pl.ds(0, half), pl.ds(half, half))

    def send_route(src, dst, peer):
        return (send(idxs.at[src], idxs.at[dst], peer), send(gats.at[src], gats.at[dst], peer))

    def send_rows(src, dst, s, peer):
        return send(toks.at[src].at[halves[s]], toks.at[dst].at[halves[s]], peer)

    def wait_all(copies):
        for copy in copies:
            copy.wait_recv()

    r_x = send_route((OWN, 0), (XN, 0), to_x)
    r_y = send_route((OWN, 0), (YN, 0), to_y)
    r_c = send_route((OWN, 0), (OWN, 1), to_c)
    t_x0 = send_rows((OWN, 0), (XN, 0), 0, to_x)
    t_y1 = send_rows((OWN, 0), (YN, 0), 1, to_y)
    t_x1 = send_rows((OWN, 0), (XN, 0), 1, to_x)
    t_y0 = send_rows((OWN, 0), (YN, 0), 0, to_y)

    sub16 = lax.broadcasted_iota(jnp.int32, (16, rows), 0)
    exp_id = jnp.where(sub16 < 8, base_own + sub16, base_par + sub16 - 8)
    row_i = lax.broadcasted_iota(jnp.int32, (rows, rows), 0)
    col_i = lax.broadcasted_iota(jnp.int32, (rows, rows), 1)
    before = jnp.where((row_i < col_i) & ((row_i < half) == (col_i < half)), 1.0, 0.0).astype(BF16)
    place = lax.broadcasted_iota(jnp.int32, (SLOT, rows), 0).astype(F32)

    def prepare(chip, core):
        idx, gat = idxs[chip, core], gats[chip, core]
        chosen = jnp.zeros((16, rows), F32)
        weight = jnp.zeros((16, rows), F32)
        for j in range(top_k):
            hit = jnp.broadcast_to(idx[j:j + 1, :], (16, rows)) == exp_id
            chosen = jnp.where(hit, 1.0, chosen)
            weight = jnp.where(hit, jnp.broadcast_to(gat[j:j + 1, :], (16, rows)), weight)
        rank = jnp.dot(chosen.astype(BF16), before, preferred_element_type=F32)
        rank = jnp.where(chosen > 0.0, rank, -1.0)
        for s in (0, 1):
            part_rank = rank[:, s * half:(s + 1) * half]
            for e in range(n_exp):
                here = jnp.broadcast_to(part_rank[e:e + 1, :], (SLOT, half)) == place[:, :half]
                pick[chip, core, s, pl.ds(e * SLOT, SLOT), :] = jnp.where(here, 1.0, 0.0).astype(BF16)
        if core == 0:
            cols = []
            for k in range(2 * n_exp):
                row = k if k < n_exp else 8 + k - n_exp
                here = jnp.broadcast_to(rank[row:row + 1, :], (SLOT, rows)) == place
                cols.append(jnp.where(here, jnp.broadcast_to(weight[row:row + 1, :], (SLOT, rows)), 0.0))
            full = jnp.concatenate(cols, axis=0).T
            first = full.astype(BF16)
            rest = full - first.astype(F32)
            second = rest.astype(BF16)
            mix[chip, 0] = first
            mix[chip, 1] = second
            mix[chip, 2] = (rest - second.astype(F32)).astype(BF16)

    def gather(k, chip, core, s):
        for n in range(PIECES):
            cols = pl.ds(n * width, width)
            got = jnp.dot(
                pick[chip, core, s], toks[chip, core, halves[s], cols], preferred_element_type=F32
            ).astype(BF16)
            for e in range(n_exp):
                xg[e, pl.ds(k * SLOT, SLOT), cols] = got[e * SLOT:(e + 1) * SLOT, :]

    def up_gate(e):
        a = jnp.dot(xg[e], wg[e], preferred_element_type=F32)
        b = jnp.dot(xg[e], wu[e], preferred_element_type=F32)
        hid[e] = (jax.nn.silu(a) * b).astype(BF16)

    def down(group, n):
        for e in range(n_exp):
            y = jnp.dot(hid[e], wd[e, :, pl.ds(n * width, width)], preferred_element_type=F32).astype(BF16)
            for k, (chip, core, s) in enumerate(group):
                piece = y[k * SLOT:(k + 1) * SLOT, :]
                dst = ys if core else yc
                dst[chip, s, n, pl.ds(e * SLOT, SLOT), :] = piece
        return [
            send(ys.at[chip, s, n], yc.at[chip, s, n].at[pl.ds(n_slot, n_slot)], to_c)
            for chip, core, s in group if core
        ]

    def combine(chip, s, n):
        y = yc[chip, s, n]
        total = jnp.dot(mix[chip, 2, halves[s]], y, preferred_element_type=F32)
        total += jnp.dot(mix[chip, 1, halves[s]], y, preferred_element_type=F32)
        total += jnp.dot(mix[chip, 0, halves[s]], y, preferred_element_type=F32)
        part[chip, s, n] = total

    def finish(group, after):
        targets = [(chip, s) for chip, core, s in group if core]
        held = down(group, 0)
        for n in range(PIECES):
            nxt = down(group, n + 1) if n + 1 < PIECES else None
            for copy, (chip, s) in zip(held, targets):
                copy.wait_recv()
                combine(chip, s, n)
                after(chip, s, n)
            held = nxt

    fin = {}
    rel = {}

    def send_sum(chip, s, n):
        dst, peer = (finx, to_x) if chip == XN else (finy, to_y)
        fin[chip, s, n] = send(part.at[chip, s, n], dst.at[s, n], peer)

    def send_far(chip, s, n):
        dst, peer = (rely, to_y) if s else (relx, to_x)
        rel[s, n] = send(part.at[chip, s, n], dst.at[n], peer)

    def relay(n):
        for s, chip, src in ((0, YN, relx), (1, XN, rely)):
            rel[s, n].wait_recv()
            part[chip, s, n] += src[n]
            send_sum(chip, s, n)

    def nothing(chip, s, n):
        pass

    wait_all(r_x)
    r_xc = send_route((XN, 0), (XN, 1), to_c)
    r_d = send_route((XN, 0), (DG, 0), to_y)
    wait_all(r_y)
    r_yc = send_route((YN, 0), (YN, 1), to_c)
    prepare(XN, 0)
    prepare(YN, 0)
    wait_all(r_xc)
    prepare(XN, 1)
    wait_all(r_yc)
    prepare(YN, 1)
    wait_all(r_d)
    r_dc = send_route((DG, 0), (DG, 1), to_c)

    t_x0.wait_recv()
    t_d0 = send_rows((XN, 0), (DG, 0), 0, to_y)
    t_xc0 = send_rows((XN, 0), (XN, 1), 0, to_c)
    t_y1.wait_recv()
    t_d1 = send_rows((YN, 0), (DG, 0), 1, to_x)
    t_yc1 = send_rows((YN, 0), (YN, 1), 1, to_c)
    t_c = send(toks.at[OWN, 0], toks.at[OWN, 1], to_c)

    gather(0, *FIRST[0])
    gather(2, *FIRST[2])
    t_xc0.wait_recv()
    gather(1, *FIRST[1])
    t_yc1.wait_recv()
    gather(3, *FIRST[3])
    for e in range(n_exp):
        loads["g", e].wait()
        loads["u", e].wait()
        up_gate(e)
    for e in range(n_exp):
        loads["d", e].wait()
    finish(FIRST, send_sum)

    t_x1.wait_recv()
    t_xc1 = send_rows((XN, 0), (XN, 1), 1, to_c)
    t_y0.wait_recv()
    t_yc0 = send_rows((YN, 0), (YN, 1), 0, to_c)
    prepare(DG, 0)
    wait_all(r_dc)
    prepare(DG, 1)
    t_d0.wait_recv()
    t_dc0 = send_rows((DG, 0), (DG, 1), 0, to_c)
    t_d1.wait_recv()
    t_dc1 = send_rows((DG, 0), (DG, 1), 1, to_c)
    gather(0, *SECOND[0])
    gather(2, *SECOND[2])
    t_dc0.wait_recv()
    gather(1, *SECOND[1])
    t_dc1.wait_recv()
    gather(3, *SECOND[3])
    for e in range(n_exp):
        up_gate(e)
    finish(SECOND, send_far)

    gather(0, *THIRD[0])
    gather(2, *THIRD[2])
    t_xc1.wait_recv()
    gather(1, *THIRD[1])
    t_yc0.wait_recv()
    gather(3, *THIRD[3])
    for e in range(n_exp):
        up_gate(e)
    finish(THIRD, nothing)

    prepare(OWN, 0)
    wait_all(r_c)
    prepare(OWN, 1)
    relay(0)
    t_c.wait_recv()
    for k in range(4):
        gather(k, *LAST[k])
    for e in range(n_exp):
        up_gate(e)
    relay(1)
    finish(LAST, nothing)
    relay(2)

    for n in range(PIECES):
        cols = pl.ds(n * width, width)
        for s in (0, 1):
            part[OWN, s, n] += toks[OWN, 0, halves[s], cols].astype(F32)
    for n in range(PIECES):
        for s in (0, 1):
            fin[XN, s, n].wait_recv()
            fin[YN, s, n].wait_recv()
            out_ref[halves[s], pl.ds(n * width, width)] = (
                part[OWN, s, n] + finx[s, n] + finy[s, n]
            ).astype(BF16)
    for copy in sent:
        copy.wait_send()


def solution(mesh):
    row_spec = P(('dp', 'ep2', 'ep'), None)
    weight_spec = P(('ep2', 'ep'), None, None)

    def local_step(tokens, expert_idx, gates, w_gate, w_up, w_down):
        rows, d_model = tokens.shape
        top_k = expert_idx.shape[1]
        n_exp, _, d_ff = w_gate.shape
        width = d_model // PIECES
        n_slot = n_exp * SLOT
        half = rows // 2
        hbm = pl.BlockSpec(memory_space=pl.ANY)
        n_sem = 80
        args = (tokens, expert_idx.T, gates.T, w_gate, w_up, w_down)
        args = [pltpu.with_memory_space_constraint(a, pltpu.HBM) for a in args]
        return pl.pallas_call(
            moe_kernel,
            out_shape=jax.ShapeDtypeStruct((rows, d_model), BF16),
            in_specs=[hbm] * 6,
            out_specs=pl.BlockSpec(memory_space=pltpu.VMEM),
            scratch_shapes=[
                pltpu.VMEM((n_exp, d_model, d_ff), BF16),
                pltpu.VMEM((n_exp, d_model, d_ff), BF16),
                pltpu.VMEM((n_exp, d_ff, d_model), BF16),
                pltpu.VMEM((4, 2, rows, d_model), BF16),
                pltpu.VMEM((4, 2, top_k, rows), jnp.int32),
                pltpu.VMEM((4, 2, top_k, rows), F32),
                pltpu.VMEM((4, 2, 2, n_slot, half), BF16),
                pltpu.VMEM((4, 3, rows, 2 * n_slot), BF16),
                pltpu.VMEM((n_exp, 4 * SLOT, d_model), BF16),
                pltpu.VMEM((n_exp, 4 * SLOT, d_ff), BF16),
                pltpu.VMEM((4, 2, PIECES, 2 * n_slot, width), BF16),
                pltpu.VMEM((4, 2, PIECES, n_slot, width), BF16),
                pltpu.VMEM((4, 2, PIECES, half, width), F32),
                pltpu.VMEM((PIECES, half, width), F32),
                pltpu.VMEM((PIECES, half, width), F32),
                pltpu.VMEM((2, PIECES, half, width), F32),
                pltpu.VMEM((2, PIECES, half, width), F32),
                pltpu.SemaphoreType.DMA((3,)),
                pltpu.SemaphoreType.DMA((3 * n_exp,)),
                pltpu.SemaphoreType.DMA((n_sem,)),
                pltpu.SemaphoreType.DMA((n_sem,)),
            ],
            compiler_params=pltpu.CompilerParams(
                collective_id=0, has_side_effects=True, vmem_limit_bytes=50 * 1024 * 1024
            ),
            name="moe",
        )(*args)

    return jax.shard_map(
        local_step, mesh=mesh,
        in_specs=(row_spec, row_spec, row_spec, weight_spec, weight_spec, weight_spec),
        out_specs=row_spec, check_vma=False,
    )
```

```python
import itertools

import jax
import jax.numpy as jnp
from jax import lax
from jax.experimental import pallas as pl
from jax.experimental.pallas import tpu as pltpu
from jax.sharding import PartitionSpec as P

MESH = pl.DeviceIdType.MESH
F32 = jnp.float32
BF16 = jnp.bfloat16
OWN, XN, YN, DG = 0, 1, 2, 3
SLOT = 32
UNITS = ((XN, 0, 64), (YN, 64, 64), (DG, 0, 128), (OWN, 0, 128), (XN, 64, 64), (YN, 0, 64))
PIECES = 3


def moe_kernel(
    tok_hbm, idx_hbm, gate_hbm, wg_hbm, wu_hbm, wd_hbm, out_ref,
    wg, wu, wd, toks, idxs, gats, pick, mix, xg, hid, yc, ys, part, relb, finx, finy,
    lsem, ssem, rsem,
):
    n_exp = wg.shape[0]
    rows, d_model = out_ref.shape
    half = rows // 2
    width = d_model // PIECES
    n_slot = n_exp * SLOT
    top_k = idx_hbm.shape[0]

    def at(chip, core):
        return chip * 2 + core

    me = at(OWN, 0)
    own = [
        pltpu.make_async_copy(idx_hbm, idxs.at[me], lsem.at[0]),
        pltpu.make_async_copy(gate_hbm, gats.at[me], lsem.at[1]),
        pltpu.make_async_copy(tok_hbm, toks.at[me], lsem.at[2]),
    ]
    for copy in own:
        copy.start()
    loads = [
        pltpu.make_async_copy(src, dst, lsem.at[3 + i])
        for i, (src, dst) in enumerate(((wg_hbm, wg), (wu_hbm, wu), (wd_hbm, wd)))
    ]

    iy = lax.axis_index("ep2")
    ie = lax.axis_index("ep")
    ix = ie // 2
    ic = ie % 2
    to_x = {"ep2": iy, "ep": (1 - ix) * 2 + ic}
    to_y = {"ep2": 1 - iy, "ep": ie}
    to_c = {"ep2": iy, "ep": ix * 2 + 1 - ic}
    base_own = (iy * 4 + ie) * n_exp
    base_par = (iy * 4 + ix * 2 + 1 - ic) * n_exp

    barrier = pltpu.get_barrier_semaphore()
    for peer in (to_x, to_y, to_c):
        pl.semaphore_signal(barrier, inc=1, device_id=peer, device_id_type=MESH)
    for copy in loads:
        copy.start()
    for copy in own:
        copy.wait()
    pl.semaphore_wait(barrier, 3)

    ids = itertools.count()

    def new_sem():
        return rsem.at[next(ids)]

    def send(src, dst, peer, kind, sem):
        pltpu.make_async_remote_copy(
            src_ref=src, dst_ref=dst, send_sem=ssem.at[kind], recv_sem=sem,
            device_id=peer, device_id_type=MESH,
        ).start()

    def arrived(sem, like):
        pltpu.make_async_copy(like, like, sem).wait()

    def send_route(src, dst, peer):
        sem = new_sem()
        send(idxs.at[src], idxs.at[dst], peer, 0, sem)
        send(gats.at[src], gats.at[dst], peer, 1, sem)
        return lambda: arrived(sem, gats.at[pl.ds(0, 2)])

    def send_rows(src, dst, first, peer, count=half):
        sem = new_sem()
        span = pl.ds(first, count)
        send(toks.at[src].at[span], toks.at[dst].at[span], peer, 2, sem)
        return lambda: arrived(sem, toks.at[dst].at[span])

    r_x = send_route(me, at(XN, 0), to_x)
    r_y = send_route(me, at(YN, 0), to_y)
    r_c = send_route(me, at(OWN, 1), to_c)
    t_x0 = send_rows(me, at(XN, 0), 0, to_x)
    t_y1 = send_rows(me, at(YN, 0), half, to_y)

    sub16 = lax.broadcasted_iota(jnp.int32, (16, rows), 0)
    exp_id = jnp.where(sub16 < 8, base_own + sub16, base_par + sub16 - 8)
    row_i = lax.broadcasted_iota(jnp.int32, (rows, rows), 0)
    col_i = lax.broadcasted_iota(jnp.int32, (rows, rows), 1)
    before = jnp.where(row_i < col_i, 1.0, 0.0).astype(BF16)
    before_half = jnp.where((row_i < col_i) & ((row_i < half) == (col_i < half)), 1.0, 0.0).astype(BF16)
    place = lax.broadcasted_iota(jnp.int32, (SLOT, rows), 0).astype(F32)

    def prepare(chip, core):
        idx, gat = idxs[at(chip, core)], gats[at(chip, core)]
        chosen = jnp.zeros((16, rows), F32)
        weight = jnp.zeros((16, rows), F32)
        for j in range(top_k):
            hit = jnp.broadcast_to(idx[j:j + 1, :], (16, rows)) == exp_id
            chosen = jnp.where(hit, 1.0, chosen)
            weight = jnp.where(hit, jnp.broadcast_to(gat[j:j + 1, :], (16, rows)), weight)
        units = [(u, first, count) for u, (c, first, count) in enumerate(UNITS) if c == chip]
        order = before if len(units) == 1 else before_half
        rank = jnp.dot(chosen.astype(BF16), order, preferred_element_type=F32)
        rank = jnp.where(chosen > 0.0, rank, -1.0)
        for u, first, count in units:
            unit_rank = rank[:, first:first + count]
            for e in range(n_exp):
                here = jnp.broadcast_to(unit_rank[e:e + 1, :], (SLOT, count)) == place[:, :count]
                pick[u, core, pl.ds(e * SLOT, SLOT), pl.ds(0, count)] = jnp.where(here, 1.0, 0.0).astype(BF16)
        if core == 0:
            cols = []
            for k in range(2 * n_exp):
                row = k if k < n_exp else 8 + k - n_exp
                here = jnp.broadcast_to(rank[row:row + 1, :], (SLOT, rows)) == place
                cols.append(jnp.where(here, jnp.broadcast_to(weight[row:row + 1, :], (SLOT, rows)), 0.0))
            full = jnp.concatenate(cols, axis=0).T
            terms = [full.astype(BF16)]
            rest = full - terms[0].astype(F32)
            terms.append(rest.astype(BF16))
            terms.append((rest - terms[1].astype(F32)).astype(BF16))
            for u, first, count in units:
                for t in range(3):
                    mix[u, t, pl.ds(0, count), :] = terms[t][first:first + count, :]

    def gather(k, u, core):
        chip, first, count = UNITS[u]
        for n in range(PIECES):
            cols = pl.ds(n * width, width)
            got = jnp.dot(
                pick[u, core, :, pl.ds(0, count)], toks[at(chip, core), pl.ds(first, count), cols],
                preferred_element_type=F32,
            ).astype(BF16)
            for e in range(n_exp):
                xg[e, pl.ds(k * SLOT, SLOT), cols] = got[e * SLOT:(e + 1) * SLOT, :]

    def up_gate():
        for e in range(n_exp):
            a = jnp.dot(xg[e], wg[e], preferred_element_type=F32)
            b = jnp.dot(xg[e], wu[e], preferred_element_type=F32)
            hid[e] = (jax.nn.silu(a) * b).astype(BF16)

    def down(group, n, sems):
        for e in range(n_exp):
            y = jnp.dot(hid[e], wd[e, :, pl.ds(n * width, width)], preferred_element_type=F32).astype(BF16)
            for k, (u, core) in enumerate(group):
                dst = ys if core else yc
                dst[u, n, pl.ds(e * SLOT, SLOT), :] = y[k * SLOT:(k + 1) * SLOT, :]
        for u, core in group:
            if core:
                send(ys.at[u, n], yc.at[u, n].at[pl.ds(n_slot, n_slot)], to_c, 3, sems[u])

    def combine(u, n):
        chip, first, count = UNITS[u]
        y = yc[u, n]
        total = jnp.dot(mix[u, 2, pl.ds(0, count)], y, preferred_element_type=F32)
        total += jnp.dot(mix[u, 1, pl.ds(0, count)], y, preferred_element_type=F32)
        total += jnp.dot(mix[u, 0, pl.ds(0, count)], y, preferred_element_type=F32)
        for s in (0, 1):
            if first <= s * half < first + count:
                part[chip, s * PIECES + n] = total[s * half - first:(s + 1) * half - first, :]

    def send_sum(chip, s, n, sem):
        dst, peer = (finx, to_x) if chip == XN else (finy, to_y)
        send(part.at[chip, s * PIECES + n], dst.at[s, n], peer, 4, sem)

    r_x()
    r_xc = send_route(at(XN, 0), at(XN, 1), to_c)
    r_d = send_route(at(XN, 0), at(DG, 0), to_y)
    r_y()
    r_yc = send_route(at(YN, 0), at(YN, 1), to_c)
    t_x1 = send_rows(me, at(XN, 0), half, to_x)
    t_y0 = send_rows(me, at(YN, 0), 0, to_y)
    prepare(XN, 0)
    prepare(YN, 0)
    r_xc()
    prepare(XN, 1)
    r_yc()
    prepare(YN, 1)
    prepare(OWN, 0)
    r_c()
    prepare(OWN, 1)

    t_x0()
    t_d0 = send_rows(at(XN, 0), at(DG, 0), 0, to_y)
    t_xc0 = send_rows(at(XN, 0), at(XN, 1), 0, to_c)
    t_y1()
    t_d1 = send_rows(at(YN, 0), at(DG, 0), half, to_x)
    t_yc1 = send_rows(at(YN, 0), at(YN, 1), half, to_c)
    r_d()
    r_dc = send_route(at(DG, 0), at(DG, 1), to_c)
    t_c = send_rows(me, at(OWN, 1), 0, to_c, rows)

    group = ((0, 0), (0, 1), (1, 0), (1, 1))
    gather(0, *group[0])
    gather(2, *group[2])
    prepare(DG, 0)
    t_xc0()
    gather(1, *group[1])
    t_yc1()
    gather(3, *group[3])
    loads[0].wait()
    loads[1].wait()
    up_gate()
    loads[2].wait()
    sems = [new_sem() for _ in range(PIECES)]
    fin_first = new_sem()
    for n in range(PIECES):
        down(group, n, {0: sems[n], 1: sems[n]})
    for n in range(PIECES):
        arrived(sems[n], ys.at[pl.ds(0, 2), n])
        combine(0, n)
        send_sum(XN, 0, n, fin_first)
        combine(1, n)
        send_sum(YN, 1, n, fin_first)

    t_x1()
    t_xc1 = send_rows(at(XN, 0), at(XN, 1), half, to_c)
    t_y0()
    t_yc0 = send_rows(at(YN, 0), at(YN, 1), 0, to_c)
    r_dc()
    prepare(DG, 1)
    group = ((2, 0), (2, 1), (3, 0), (3, 1))
    gather(2, *group[2])
    t_c()
    gather(3, *group[3])
    t_d0()
    t_dc0 = send_rows(at(DG, 0), at(DG, 1), 0, to_c)
    t_d1()
    t_dc1 = send_rows(at(DG, 0), at(DG, 1), half, to_c)
    gather(0, *group[0])
    t_dc0()
    t_dc1()
    gather(1, *group[1])
    up_gate()
    sems = [new_sem() for _ in range(PIECES)]
    own_sem = new_sem()
    far = [new_sem() for _ in range(PIECES)]
    for n in range(PIECES):
        down(group, n, {2: sems[n], 3: own_sem})
    for n in range(PIECES):
        arrived(sems[n], ys.at[2, n])
        combine(2, n)
        send(part.at[DG, n], relb.at[0, n], to_x, 4, far[n])
        send(part.at[DG, PIECES + n], relb.at[1, n], to_y, 4, far[n])

    group = ((4, 0), (4, 1), (5, 0), (5, 1))
    t_xc1()
    t_yc0()
    for k in range(4):
        gather(k, *group[k])
    up_gate()
    sems = [new_sem() for _ in range(PIECES)]
    fin_last = [new_sem() for _ in range(PIECES)]
    for n in range(PIECES):
        down(group, n, {4: sems[n], 5: sems[n]})
    for n in range(PIECES):
        arrived(sems[n], ys.at[pl.ds(4, 2), n])
        combine(4, n)
        combine(5, n)

    for n in range(PIECES):
        arrived(far[n], relb.at[:, n])
        part[YN, n] += relb[0, n]
        send_sum(YN, 0, n, fin_last[n])
        part[XN, PIECES + n] += relb[1, n]
        send_sum(XN, 1, n, fin_last[n])
        if n == 0:
            arrived(own_sem, ys.at[3])
            for m in range(PIECES):
                combine(3, m)
                for s in (0, 1):
                    part[OWN, s * PIECES + m] += toks[
                        me, pl.ds(s * half, half), pl.ds(m * width, width)
                    ].astype(F32)

    arrived(fin_first, finx)
    for n in range(PIECES):
        arrived(fin_last[n], finx.at[:, n])
        for s in (0, 1):
            out_ref[pl.ds(s * half, half), pl.ds(n * width, width)] = (
                part[OWN, s * PIECES + n] + finx[s, n] + finy[s, n]
            ).astype(BF16)
    arrived(ssem.at[0], idxs.at[pl.ds(0, 7)])
    arrived(ssem.at[1], gats.at[pl.ds(0, 7)])
    arrived(ssem.at[2], toks.at[pl.ds(0, 7)])
    arrived(ssem.at[3], ys)
    arrived(ssem.at[4], part.at[pl.ds(0, 3)])


def solution(mesh):
    row_spec = P(('dp', 'ep2', 'ep'), None)
    weight_spec = P(('ep2', 'ep'), None, None)

    def local_step(tokens, expert_idx, gates, w_gate, w_up, w_down):
        rows, d_model = tokens.shape
        top_k = expert_idx.shape[1]
        n_exp, _, d_ff = w_gate.shape
        width = d_model // PIECES
        n_slot = n_exp * SLOT
        half = rows // 2
        hbm = pl.BlockSpec(memory_space=pl.ANY)
        n_sem = 22 + 5 * PIECES
        args = (tokens, expert_idx.T, gates.T, w_gate, w_up, w_down)
        args = [pltpu.with_memory_space_constraint(a, pltpu.HBM) for a in args]
        return pl.pallas_call(
            moe_kernel,
            out_shape=jax.ShapeDtypeStruct((rows, d_model), BF16),
            in_specs=[hbm] * 6,
            out_specs=pl.BlockSpec(memory_space=pltpu.VMEM),
            scratch_shapes=[
                pltpu.VMEM((n_exp, d_model, d_ff), BF16),
                pltpu.VMEM((n_exp, d_model, d_ff), BF16),
                pltpu.VMEM((n_exp, d_ff, d_model), BF16),
                pltpu.VMEM((8, rows, d_model), BF16),
                pltpu.VMEM((8, top_k, rows), jnp.int32),
                pltpu.VMEM((8, top_k, rows), F32),
                pltpu.VMEM((len(UNITS), 2, n_slot, rows), BF16),
                pltpu.VMEM((len(UNITS), 3, rows, 2 * n_slot), BF16),
                pltpu.VMEM((n_exp, 4 * SLOT, d_model), BF16),
                pltpu.VMEM((n_exp, 4 * SLOT, d_ff), BF16),
                pltpu.VMEM((len(UNITS), PIECES, 2 * n_slot, width), BF16),
                pltpu.VMEM((len(UNITS), PIECES, n_slot, width), BF16),
                pltpu.VMEM((4, 2 * PIECES, half, width), F32),
                pltpu.VMEM((2, PIECES, half, width), F32),
                pltpu.VMEM((2, PIECES, half, width), F32),
                pltpu.VMEM((2, PIECES, half, width), F32),
                pltpu.SemaphoreType.DMA((6,)),
                pltpu.SemaphoreType.DMA((5,)),
                pltpu.SemaphoreType.DMA((n_sem,)),
            ],
            compiler_params=pltpu.CompilerParams(
                collective_id=0, has_side_effects=True, vmem_limit_bytes=50 * 1024 * 1024
            ),
            name="moe",
        )(*args)

    return jax.shard_map(
        local_step, mesh=mesh,
        in_specs=(row_spec, row_spec, row_spec, weight_spec, weight_spec, weight_spec),
        out_specs=row_spec, check_vma=False,
    )
```

```python
import itertools

import jax
import jax.numpy as jnp
from jax import lax
from jax.experimental import pallas as pl
from jax.experimental.pallas import tpu as pltpu
from jax.sharding import PartitionSpec as P

MESH = pl.DeviceIdType.MESH
F32 = jnp.float32
BF16 = jnp.bfloat16
OWN, XN, YN, DG = 0, 1, 2, 3
SLOT = 32
UNITS = ((XN, 0, 64), (YN, 64, 64), (DG, 0, 128), (OWN, 0, 128), (XN, 64, 64), (YN, 0, 64))
EARLY = 32
PIECES = 3
BF16_MAX = float(jnp.finfo(jnp.bfloat16).max)


def moe_kernel(
    tok_hbm, idx_hbm, gate_hbm, wg_hbm, wu_hbm, wd_hbm, out_ref,
    wg, wu, wd, toks, idxs, gats, pick, mix, xg, hid, yc, ys, part, relb, finx, finy,
    lsem, ssem, rsem,
):
    n_exp = wg.shape[0]
    rows, d_model = out_ref.shape
    half = rows // 2
    width = d_model // PIECES
    n_slot = n_exp * SLOT
    top_k = idx_hbm.shape[0]

    def at(chip, core):
        return chip * 2 + core

    me = at(OWN, 0)
    own = [
        pltpu.make_async_copy(idx_hbm, idxs.at[me], lsem.at[0]),
        pltpu.make_async_copy(gate_hbm, gats.at[me], lsem.at[1]),
        pltpu.make_async_copy(tok_hbm, toks.at[me], lsem.at[2]),
    ]
    for copy in own:
        copy.start()
    loads = [
        pltpu.make_async_copy(src, dst, lsem.at[3 + i])
        for i, (src, dst) in enumerate(((wg_hbm, wg), (wu_hbm, wu), (wd_hbm, wd)))
    ]

    iy = lax.axis_index("ep2")
    ie = lax.axis_index("ep")
    ix = ie // 2
    ic = ie % 2
    to_x = {"ep2": iy, "ep": (1 - ix) * 2 + ic}
    to_y = {"ep2": 1 - iy, "ep": ie}
    to_c = {"ep2": iy, "ep": ix * 2 + 1 - ic}
    base_own = (iy * 4 + ie) * n_exp
    base_par = (iy * 4 + ix * 2 + 1 - ic) * n_exp

    barrier = pltpu.get_barrier_semaphore()
    for peer in (to_x, to_y, to_c):
        pl.semaphore_signal(barrier, inc=1, device_id=peer, device_id_type=MESH)
    for copy in loads:
        copy.start()
    for copy in own:
        copy.wait()
    pl.semaphore_wait(barrier, 3)

    ids = itertools.count()

    def new_sem():
        return rsem.at[next(ids)]

    def send(src, dst, peer, kind, sem):
        pltpu.make_async_remote_copy(
            src_ref=src, dst_ref=dst, send_sem=ssem.at[kind], recv_sem=sem,
            device_id=peer, device_id_type=MESH,
        ).start()

    def arrived(sem, like):
        pltpu.make_async_copy(like, like, sem).wait()

    def send_route(src, dst, peer):
        sem = new_sem()
        send(idxs.at[src], idxs.at[dst], peer, 0, sem)
        send(gats.at[src], gats.at[dst], peer, 1, sem)
        return lambda: arrived(sem, gats.at[pl.ds(0, 2)])

    def start_rows(src, dst, first, count, peer, sem):
        span = pl.ds(first, count)
        send(toks.at[src].at[span], toks.at[dst].at[span], peer, 2, sem)

    def send_rows(src, dst, first, peer, count=half):
        sem = new_sem()
        start_rows(src, dst, first, count, peer, sem)
        return lambda: arrived(sem, toks.at[dst].at[pl.ds(first, count)])

    r_x = send_route(me, at(XN, 0), to_x)
    r_y = send_route(me, at(YN, 0), to_y)
    r_c = send_route(me, at(OWN, 1), to_c)
    t_x0 = send_rows(me, at(XN, 0), 0, to_x)
    t_y1 = send_rows(me, at(YN, 0), half, to_y)

    sub16 = lax.broadcasted_iota(jnp.int32, (16, rows), 0)
    exp_id = jnp.where(sub16 < 8, base_own + sub16, base_par + sub16 - 8)
    row_i = lax.broadcasted_iota(jnp.int32, (rows, rows), 0)
    col_i = lax.broadcasted_iota(jnp.int32, (rows, rows), 1)
    before = jnp.where(row_i < col_i, 1.0, 0.0).astype(BF16)
    before_half = jnp.where((row_i < col_i) & ((row_i < half) == (col_i < half)), 1.0, 0.0).astype(BF16)
    place = lax.broadcasted_iota(jnp.int32, (SLOT, rows), 0).astype(F32)

    def prepare(chip, core):
        idx, gat = idxs[at(chip, core)], gats[at(chip, core)]
        chosen = jnp.zeros((16, rows), F32)
        weight = jnp.zeros((16, rows), F32)
        for j in range(top_k):
            hit = jnp.broadcast_to(idx[j:j + 1, :], (16, rows)) == exp_id
            chosen = jnp.where(hit, 1.0, chosen)
            weight = jnp.where(hit, jnp.broadcast_to(gat[j:j + 1, :], (16, rows)), weight)
        units = [(u, first, count) for u, (c, first, count) in enumerate(UNITS) if c == chip]
        order = before if len(units) == 1 else before_half
        rank = jnp.dot(chosen.astype(BF16), order, preferred_element_type=F32)
        rank = jnp.where(chosen > 0.0, rank, -1.0)
        for u, first, count in units:
            unit_rank = rank[:, first:first + count]
            for e in range(n_exp):
                here = jnp.broadcast_to(unit_rank[e:e + 1, :], (SLOT, count)) == place[:, :count]
                pick[u, core, pl.ds(e * SLOT, SLOT), pl.ds(0, count)] = jnp.where(here, 1.0, 0.0).astype(BF16)
        if core == 0:
            cols = []
            for k in range(2 * n_exp):
                row = k if k < n_exp else 8 + k - n_exp
                here = jnp.broadcast_to(rank[row:row + 1, :], (SLOT, rows)) == place
                cols.append(jnp.where(here, jnp.broadcast_to(weight[row:row + 1, :], (SLOT, rows)), 0.0))
            full = jnp.concatenate(cols, axis=0).T
            terms = [jnp.minimum(full, BF16_MAX).astype(BF16)]
            rest = full - terms[0].astype(F32)
            terms.append(rest.astype(BF16))
            terms.append((rest - terms[1].astype(F32)).astype(BF16))
            for u, first, count in units:
                for t in range(3):
                    mix[u, t, pl.ds(0, count), :] = terms[t][first:first + count, :]

    def gather(k, u, core):
        chip, first, count = UNITS[u]
        for n in range(PIECES):
            cols = pl.ds(n * width, width)
            got = jnp.dot(
                pick[u, core, :, pl.ds(0, count)], toks[at(chip, core), pl.ds(first, count), cols],
                preferred_element_type=F32,
            ).astype(BF16)
            for e in range(n_exp):
                xg[e, pl.ds(k * SLOT, SLOT), cols] = got[e * SLOT:(e + 1) * SLOT, :]

    def up_gate():
        for e in range(n_exp):
            a = jnp.dot(xg[e], wg[e], preferred_element_type=F32)
            b = jnp.dot(xg[e], wu[e], preferred_element_type=F32)
            hid[e] = (jax.nn.silu(a) * b).astype(BF16)

    def down(group, n, sems):
        for e in range(n_exp):
            y = jnp.dot(hid[e], wd[e, :, pl.ds(n * width, width)], preferred_element_type=F32).astype(BF16)
            for k, (u, core) in enumerate(group):
                dst = ys if core else yc
                dst[u, n, pl.ds(e * SLOT, SLOT), :] = y[k * SLOT:(k + 1) * SLOT, :]
        for u, core in group:
            if core:
                send(ys.at[u, n], yc.at[u, n].at[pl.ds(n_slot, n_slot)], to_c, 3, sems[u])

    def combine(u, n):
        chip, first, count = UNITS[u]
        y = yc[u, n]
        total = jnp.dot(mix[u, 2, pl.ds(0, count)], y, preferred_element_type=F32)
        total += jnp.dot(mix[u, 1, pl.ds(0, count)], y, preferred_element_type=F32)
        total += jnp.dot(mix[u, 0, pl.ds(0, count)], y, preferred_element_type=F32)
        for s in (0, 1):
            if first <= s * half < first + count:
                part[chip, s * PIECES + n] = total[s * half - first:(s + 1) * half - first, :]

    def send_sum(chip, s, n, sem):
        dst, peer = (finx, to_x) if chip == XN else (finy, to_y)
        send(part.at[chip, s * PIECES + n], dst.at[s, n], peer, 4, sem)

    r_x()
    r_xc = send_route(at(XN, 0), at(XN, 1), to_c)
    r_d = send_route(at(XN, 0), at(DG, 0), to_y)
    r_y()
    r_yc = send_route(at(YN, 0), at(YN, 1), to_c)
    prepare(XN, 0)
    prepare(YN, 0)
    r_xc()
    prepare(XN, 1)
    sem_x1, sem_y0 = new_sem(), new_sem()
    start_rows(me, at(XN, 0), half, EARLY, to_x, sem_x1)
    start_rows(me, at(YN, 0), 0, EARLY, to_y, sem_y0)
    r_yc()
    prepare(YN, 1)
    prepare(OWN, 0)
    r_c()
    prepare(OWN, 1)

    t_x0()
    t_d0 = send_rows(at(XN, 0), at(DG, 0), 0, to_y)
    t_xc0 = send_rows(at(XN, 0), at(XN, 1), 0, to_c)
    t_y1()
    t_d1 = send_rows(at(YN, 0), at(DG, 0), half, to_x)
    t_yc1 = send_rows(at(YN, 0), at(YN, 1), half, to_c)
    start_rows(me, at(XN, 0), half + EARLY, half - EARLY, to_x, sem_x1)
    start_rows(me, at(YN, 0), EARLY, half - EARLY, to_y, sem_y0)
    r_d()
    r_dc = send_route(at(DG, 0), at(DG, 1), to_c)
    t_c = send_rows(me, at(OWN, 1), 0, to_c, rows)

    group = ((0, 0), (0, 1), (1, 0), (1, 1))
    gather(0, *group[0])
    gather(2, *group[2])
    prepare(DG, 0)
    t_xc0()
    gather(1, *group[1])
    t_yc1()
    gather(3, *group[3])
    loads[0].wait()
    loads[1].wait()
    up_gate()
    loads[2].wait()
    sems = [new_sem() for _ in range(PIECES)]
    fin_first = new_sem()
    for n in range(PIECES):
        down(group, n, {0: sems[n], 1: sems[n]})
    for n in range(PIECES):
        arrived(sems[n], ys.at[pl.ds(0, 2), n])
        combine(0, n)
        send_sum(XN, 0, n, fin_first)
        combine(1, n)
        send_sum(YN, 1, n, fin_first)

    r_dc()
    prepare(DG, 1)
    group = ((2, 0), (2, 1), (3, 0), (3, 1))
    gather(2, *group[2])
    t_c()
    gather(3, *group[3])
    t_d0()
    t_dc0 = send_rows(at(DG, 0), at(DG, 1), 0, to_c)
    t_d1()
    t_dc1 = send_rows(at(DG, 0), at(DG, 1), half, to_c)
    gather(0, *group[0])
    t_dc0()
    t_dc1()
    gather(1, *group[1])
    up_gate()
    arrived(sem_x1, toks.at[at(XN, 0)].at[pl.ds(half, half)])
    t_xc1 = send_rows(at(XN, 0), at(XN, 1), half, to_c)
    arrived(sem_y0, toks.at[at(YN, 0)].at[pl.ds(0, half)])
    t_yc0 = send_rows(at(YN, 0), at(YN, 1), 0, to_c)
    sems = [new_sem() for _ in range(PIECES)]
    own_sem = new_sem()
    far = [new_sem() for _ in range(PIECES)]
    for n in range(PIECES):
        down(group, n, {2: sems[n], 3: own_sem})
    for n in range(PIECES):
        arrived(sems[n], ys.at[2, n])
        combine(2, n)
        send(part.at[DG, n], relb.at[0, n], to_x, 4, far[n])
        send(part.at[DG, PIECES + n], relb.at[1, n], to_y, 4, far[n])

    group = ((4, 0), (4, 1), (5, 0), (5, 1))
    t_xc1()
    t_yc0()
    for k in range(4):
        gather(k, *group[k])
    up_gate()
    sems = [new_sem() for _ in range(PIECES)]
    fin_last = [new_sem() for _ in range(PIECES)]
    for n in range(PIECES):
        down(group, n, {4: sems[n], 5: sems[n]})
    for n in range(PIECES):
        arrived(sems[n], ys.at[pl.ds(4, 2), n])
        combine(4, n)
        combine(5, n)

    for n in range(PIECES):
        arrived(far[n], relb.at[:, n])
        part[YN, n] += relb[0, n]
        send_sum(YN, 0, n, fin_last[n])
        part[XN, PIECES + n] += relb[1, n]
        send_sum(XN, 1, n, fin_last[n])
        if n == 0:
            arrived(own_sem, ys.at[3])
            for m in range(PIECES):
                combine(3, m)
                for s in (0, 1):
                    part[OWN, s * PIECES + m] += toks[
                        me, pl.ds(s * half, half), pl.ds(m * width, width)
                    ].astype(F32)

    arrived(fin_first, finx)
    for n in range(PIECES):
        arrived(fin_last[n], finx.at[:, n])
        for s in (0, 1):
            out_ref[pl.ds(s * half, half), pl.ds(n * width, width)] = (
                part[OWN, s * PIECES + n] + finx[s, n] + finy[s, n]
            ).astype(BF16)
    arrived(ssem.at[0], idxs.at[pl.ds(0, 7)])
    arrived(ssem.at[1], gats.at[pl.ds(0, 7)])
    arrived(ssem.at[2], toks.at[pl.ds(0, 7)])
    arrived(ssem.at[3], ys)
    arrived(ssem.at[4], part.at[pl.ds(0, 3)])


def solution(mesh):
    row_spec = P(('dp', 'ep2', 'ep'), None)
    weight_spec = P(('ep2', 'ep'), None, None)

    def local_step(tokens, expert_idx, gates, w_gate, w_up, w_down):
        rows, d_model = tokens.shape
        top_k = expert_idx.shape[1]
        n_exp, _, d_ff = w_gate.shape
        width = d_model // PIECES
        n_slot = n_exp * SLOT
        half = rows // 2
        hbm = pl.BlockSpec(memory_space=pl.ANY)
        n_sem = 22 + 5 * PIECES
        args = (tokens, expert_idx.T, gates.T, w_gate, w_up, w_down)
        args = [pltpu.with_memory_space_constraint(a, pltpu.HBM) for a in args]
        return pl.pallas_call(
            moe_kernel,
            out_shape=jax.ShapeDtypeStruct((rows, d_model), BF16),
            in_specs=[hbm] * 6,
            out_specs=pl.BlockSpec(memory_space=pltpu.VMEM),
            scratch_shapes=[
                pltpu.VMEM((n_exp, d_model, d_ff), BF16),
                pltpu.VMEM((n_exp, d_model, d_ff), BF16),
                pltpu.VMEM((n_exp, d_ff, d_model), BF16),
                pltpu.VMEM((8, rows, d_model), BF16),
                pltpu.VMEM((8, top_k, rows), jnp.int32),
                pltpu.VMEM((8, top_k, rows), F32),
                pltpu.VMEM((len(UNITS), 2, n_slot, rows), BF16),
                pltpu.VMEM((len(UNITS), 3, rows, 2 * n_slot), BF16),
                pltpu.VMEM((n_exp, 4 * SLOT, d_model), BF16),
                pltpu.VMEM((n_exp, 4 * SLOT, d_ff), BF16),
                pltpu.VMEM((len(UNITS), PIECES, 2 * n_slot, width), BF16),
                pltpu.VMEM((len(UNITS), PIECES, n_slot, width), BF16),
                pltpu.VMEM((4, 2 * PIECES, half, width), F32),
                pltpu.VMEM((2, PIECES, half, width), F32),
                pltpu.VMEM((2, PIECES, half, width), F32),
                pltpu.VMEM((2, PIECES, half, width), F32),
                pltpu.SemaphoreType.DMA((6,)),
                pltpu.SemaphoreType.DMA((5,)),
                pltpu.SemaphoreType.DMA((n_sem,)),
            ],
            compiler_params=pltpu.CompilerParams(
                collective_id=0, has_side_effects=True, vmem_limit_bytes=50 * 1024 * 1024
            ),
            name="moe",
        )(*args)

    return jax.shard_map(
        local_step, mesh=mesh,
        in_specs=(row_spec, row_spec, row_spec, weight_spec, weight_spec, weight_spec),
        out_specs=row_spec, check_vma=False,
    )
```

```python
import itertools

import jax
import jax.numpy as jnp
from jax import lax
from jax.experimental import pallas as pl
from jax.experimental.pallas import tpu as pltpu
from jax.sharding import PartitionSpec as P

MESH = pl.DeviceIdType.MESH
F32 = jnp.float32
BF16 = jnp.bfloat16
OWN, XN, YN, DG = 0, 1, 2, 3
SLOT = 32
UNITS = ((XN, 0, 64), (YN, 64, 64), (DG, 0, 128), (OWN, 0, 128), (XN, 64, 64), (YN, 0, 64))
EARLY = 32
LEAD = 16
PIECES = 3
BF16_MAX = float(jnp.finfo(jnp.bfloat16).max)


def moe_kernel(
    tok_hbm, idx_hbm, gate_hbm, wg_hbm, wu_hbm, wd_hbm, out_ref,
    wg, wu, wd, toks, idxs, gats, pick, mix, xg, hid, yc, ys, part, relb, finx, finy,
    lsem, ssem, rsem,
):
    n_exp = wg.shape[0]
    rows, d_model = out_ref.shape
    half = rows // 2
    width = d_model // PIECES
    n_slot = n_exp * SLOT
    top_k = idx_hbm.shape[0]

    def at(chip, core):
        return chip * 2 + core

    me = at(OWN, 0)
    own = [
        pltpu.make_async_copy(idx_hbm, idxs.at[me], lsem.at[0]),
        pltpu.make_async_copy(gate_hbm, gats.at[me], lsem.at[1]),
        pltpu.make_async_copy(tok_hbm, toks.at[me], lsem.at[2]),
    ]
    for copy in own:
        copy.start()
    loads = [
        pltpu.make_async_copy(src, dst, lsem.at[3 + i])
        for i, (src, dst) in enumerate(((wg_hbm, wg), (wu_hbm, wu), (wd_hbm, wd)))
    ]

    iy = lax.axis_index("ep2")
    ie = lax.axis_index("ep")
    ix = ie // 2
    ic = ie % 2
    to_x = {"ep2": iy, "ep": (1 - ix) * 2 + ic}
    to_y = {"ep2": 1 - iy, "ep": ie}
    to_c = {"ep2": iy, "ep": ix * 2 + 1 - ic}
    base_own = (iy * 4 + ie) * n_exp
    base_par = (iy * 4 + ix * 2 + 1 - ic) * n_exp

    barrier = pltpu.get_barrier_semaphore()
    for peer in (to_x, to_y, to_c):
        pl.semaphore_signal(barrier, inc=1, device_id=peer, device_id_type=MESH)
    for copy in loads:
        copy.start()
    for copy in own:
        copy.wait()
    pl.semaphore_wait(barrier, 3)

    ids = itertools.count()

    def new_sem():
        return rsem.at[next(ids)]

    def send(src, dst, peer, kind, sem):
        pltpu.make_async_remote_copy(
            src_ref=src, dst_ref=dst, send_sem=ssem.at[kind], recv_sem=sem,
            device_id=peer, device_id_type=MESH,
        ).start()

    def arrived(sem, like):
        pltpu.make_async_copy(like, like, sem).wait()

    def send_route(src, dst, peer):
        sem = new_sem()
        send(idxs.at[src], idxs.at[dst], peer, 0, sem)
        send(gats.at[src], gats.at[dst], peer, 1, sem)
        return lambda: arrived(sem, gats.at[pl.ds(0, 2)])

    def start_rows(src, dst, first, count, peer, sem):
        span = pl.ds(first, count)
        send(toks.at[src].at[span], toks.at[dst].at[span], peer, 2, sem)

    def send_rows(src, dst, first, peer, count=half):
        sem = new_sem()
        start_rows(src, dst, first, count, peer, sem)
        return lambda: arrived(sem, toks.at[dst].at[pl.ds(first, count)])

    r_x = send_route(me, at(XN, 0), to_x)
    r_y = send_route(me, at(YN, 0), to_y)
    r_c = send_route(me, at(OWN, 1), to_c)
    t_x0 = send_rows(me, at(XN, 0), 0, to_x)
    t_y1 = send_rows(me, at(YN, 0), half, to_y)

    sub16 = lax.broadcasted_iota(jnp.int32, (16, rows), 0)
    exp_id = jnp.where(sub16 < 8, base_own + sub16, base_par + sub16 - 8)
    row_i = lax.broadcasted_iota(jnp.int32, (rows, rows), 0)
    col_i = lax.broadcasted_iota(jnp.int32, (rows, rows), 1)
    before = jnp.where(row_i < col_i, 1.0, 0.0).astype(BF16)
    before_half = jnp.where((row_i < col_i) & ((row_i < half) == (col_i < half)), 1.0, 0.0).astype(BF16)
    place = lax.broadcasted_iota(jnp.int32, (SLOT, rows), 0).astype(F32)

    def prepare(chip, core):
        idx, gat = idxs[at(chip, core)], gats[at(chip, core)]
        chosen = jnp.zeros((16, rows), F32)
        weight = jnp.zeros((16, rows), F32)
        for j in range(top_k):
            hit = jnp.broadcast_to(idx[j:j + 1, :], (16, rows)) == exp_id
            chosen = jnp.where(hit, 1.0, chosen)
            weight = jnp.where(hit, jnp.broadcast_to(gat[j:j + 1, :], (16, rows)), weight)
        units = [(u, first, count) for u, (c, first, count) in enumerate(UNITS) if c == chip]
        order = before if len(units) == 1 else before_half
        rank = jnp.dot(chosen.astype(BF16), order, preferred_element_type=F32)
        rank = jnp.where(chosen > 0.0, rank, -1.0)
        for u, first, count in units:
            unit_rank = rank[:, first:first + count]
            for e in range(n_exp):
                here = jnp.broadcast_to(unit_rank[e:e + 1, :], (SLOT, count)) == place[:, :count]
                pick[u, core, pl.ds(e * SLOT, SLOT), pl.ds(0, count)] = jnp.where(here, 1.0, 0.0).astype(BF16)
        if core == 0:
            cols = []
            for k in range(2 * n_exp):
                row = k if k < n_exp else 8 + k - n_exp
                here = jnp.broadcast_to(rank[row:row + 1, :], (SLOT, rows)) == place
                cols.append(jnp.where(here, jnp.broadcast_to(weight[row:row + 1, :], (SLOT, rows)), 0.0))
            full = jnp.concatenate(cols, axis=0).T
            terms = [jnp.minimum(full, BF16_MAX).astype(BF16)]
            rest = full - terms[0].astype(F32)
            terms.append(rest.astype(BF16))
            terms.append((rest - terms[1].astype(F32)).astype(BF16))
            for u, first, count in units:
                for t in range(3):
                    mix[u, t, pl.ds(0, count), :] = terms[t][first:first + count, :]

    def gather(k, u, core):
        chip, first, count = UNITS[u]
        for n in range(PIECES):
            cols = pl.ds(n * width, width)
            got = jnp.dot(
                pick[u, core, :, pl.ds(0, count)], toks[at(chip, core), pl.ds(first, count), cols],
                preferred_element_type=F32,
            ).astype(BF16)
            for e in range(n_exp):
                xg[e, pl.ds(k * SLOT, SLOT), cols] = got[e * SLOT:(e + 1) * SLOT, :]

    def up_gate():
        for e in range(n_exp):
            a = jnp.dot(xg[e], wg[e], preferred_element_type=F32)
            b = jnp.dot(xg[e], wu[e], preferred_element_type=F32)
            hid[e] = (jax.nn.silu(a) * b).astype(BF16)

    def down(group, n, sems):
        for e in range(n_exp):
            y = jnp.dot(hid[e], wd[e, :, pl.ds(n * width, width)], preferred_element_type=F32).astype(BF16)
            for k, (u, core) in enumerate(group):
                dst = ys if core else yc
                dst[u, n, pl.ds(e * SLOT, SLOT), :] = y[k * SLOT:(k + 1) * SLOT, :]
        for u, core in group:
            if core:
                send(ys.at[u, n], yc.at[u, n].at[pl.ds(n_slot, n_slot)], to_c, 3, sems[u])

    def combine(u, n):
        chip, first, count = UNITS[u]
        y = yc[u, n]
        total = jnp.dot(mix[u, 2, pl.ds(0, count)], y, preferred_element_type=F32)
        total += jnp.dot(mix[u, 1, pl.ds(0, count)], y, preferred_element_type=F32)
        total += jnp.dot(mix[u, 0, pl.ds(0, count)], y, preferred_element_type=F32)
        for s in (0, 1):
            if first <= s * half < first + count:
                part[chip, s * PIECES + n] = total[s * half - first:(s + 1) * half - first, :]

    def send_sum(chip, s, n, sem, first=0, count=half):
        dst, peer = (finx, to_x) if chip == XN else (finy, to_y)
        span = pl.ds(first, count)
        send(part.at[chip, s * PIECES + n].at[span], dst.at[s, n].at[span], peer, 4, sem)

    r_x()
    r_xc = send_route(at(XN, 0), at(XN, 1), to_c)
    r_d = send_route(at(XN, 0), at(DG, 0), to_y)
    r_y()
    r_yc = send_route(at(YN, 0), at(YN, 1), to_c)
    prepare(XN, 0)
    prepare(YN, 0)
    r_xc()
    prepare(XN, 1)
    sem_x1, sem_y0 = new_sem(), new_sem()
    start_rows(me, at(XN, 0), half, EARLY, to_x, sem_x1)
    start_rows(me, at(YN, 0), 0, EARLY, to_y, sem_y0)
    r_yc()
    prepare(YN, 1)
    prepare(OWN, 0)
    r_c()
    prepare(OWN, 1)

    t_x0()
    t_d0 = send_rows(at(XN, 0), at(DG, 0), 0, to_y)
    t_xc0 = send_rows(at(XN, 0), at(XN, 1), 0, to_c)
    t_y1()
    t_d1 = send_rows(at(YN, 0), at(DG, 0), half, to_x)
    t_yc1 = send_rows(at(YN, 0), at(YN, 1), half, to_c)
    start_rows(me, at(XN, 0), half + EARLY, half - EARLY, to_x, sem_x1)
    start_rows(me, at(YN, 0), EARLY, half - EARLY, to_y, sem_y0)
    r_d()
    r_dc = send_route(at(DG, 0), at(DG, 1), to_c)
    t_c = send_rows(me, at(OWN, 1), 0, to_c, rows)

    group = ((0, 0), (0, 1), (1, 0), (1, 1))
    gather(0, *group[0])
    gather(2, *group[2])
    prepare(DG, 0)
    t_xc0()
    gather(1, *group[1])
    t_yc1()
    gather(3, *group[3])
    loads[0].wait()
    loads[1].wait()
    up_gate()
    loads[2].wait()
    sems = [new_sem() for _ in range(PIECES)]
    fin_first = new_sem()
    for n in range(PIECES):
        down(group, n, {0: sems[n], 1: sems[n]})
    for n in range(PIECES):
        arrived(sems[n], ys.at[pl.ds(0, 2), n])
        combine(0, n)
        send_sum(XN, 0, n, fin_first)
        combine(1, n)
        send_sum(YN, 1, n, fin_first)

    r_dc()
    prepare(DG, 1)
    group = ((2, 0), (2, 1), (3, 0), (3, 1))
    gather(2, *group[2])
    t_c()
    gather(3, *group[3])
    t_d0()
    t_dc0 = send_rows(at(DG, 0), at(DG, 1), 0, to_c)
    t_d1()
    t_dc1 = send_rows(at(DG, 0), at(DG, 1), half, to_c)
    gather(0, *group[0])
    t_dc0()
    t_dc1()
    gather(1, *group[1])
    up_gate()
    arrived(sem_x1, toks.at[at(XN, 0)].at[pl.ds(half, half)])
    t_xc1 = send_rows(at(XN, 0), at(XN, 1), half, to_c)
    arrived(sem_y0, toks.at[at(YN, 0)].at[pl.ds(0, half)])
    t_yc0 = send_rows(at(YN, 0), at(YN, 1), 0, to_c)
    sems = [new_sem() for _ in range(PIECES)]
    own_sem = new_sem()
    far = [new_sem() for _ in range(PIECES)]
    for n in range(PIECES):
        down(group, n, {2: sems[n], 3: own_sem})
    for n in range(PIECES):
        arrived(sems[n], ys.at[2, n])
        combine(2, n)
        send(part.at[DG, n], relb.at[0, n], to_x, 4, far[n])
        send(part.at[DG, PIECES + n], relb.at[1, n], to_y, 4, far[n])

    group = ((4, 0), (4, 1), (5, 0), (5, 1))
    t_xc1()
    t_yc0()
    for k in range(4):
        gather(k, *group[k])
    up_gate()
    sems = [new_sem() for _ in range(PIECES)]
    fin_last = [new_sem() for _ in range(PIECES)]
    for n in range(PIECES):
        down(group, n, {4: sems[n], 5: sems[n]})
    for n in range(PIECES):
        arrived(sems[n], ys.at[pl.ds(4, 2), n])
        combine(4, n)
        combine(5, n)

    for n in range(PIECES):
        arrived(far[n], relb.at[:, n])
        part[YN, n] += relb[0, n]
        part[XN, PIECES + n] += relb[1, n]
        if n < PIECES - 1:
            send_sum(YN, 0, n, fin_last[n])
            send_sum(XN, 1, n, fin_last[n])
        else:
            send_sum(YN, 0, n, fin_last[n], 0, LEAD)
            send_sum(XN, 1, n, fin_last[n], 0, LEAD)
            pl.when(ic == 1)(lambda: arrived(fin_last[n - 1], finx.at[:, n - 1]))
            send_sum(YN, 0, n, fin_last[n], LEAD, half - LEAD)
            send_sum(XN, 1, n, fin_last[n], LEAD, half - LEAD)
        if n == 0:
            arrived(own_sem, ys.at[3])
            for m in range(PIECES):
                combine(3, m)
                for s in (0, 1):
                    part[OWN, s * PIECES + m] += toks[
                        me, pl.ds(s * half, half), pl.ds(m * width, width)
                    ].astype(F32)

    arrived(fin_first, finx)
    for n in range(PIECES):
        if n == PIECES - 2:
            pl.when(ic == 0)(lambda: arrived(fin_last[n], finx.at[:, n]))
        else:
            arrived(fin_last[n], finx.at[:, n])
        for s in (0, 1):
            out_ref[pl.ds(s * half, half), pl.ds(n * width, width)] = (
                part[OWN, s * PIECES + n] + finx[s, n] + finy[s, n]
            ).astype(BF16)
    arrived(ssem.at[0], idxs.at[pl.ds(0, 7)])
    arrived(ssem.at[1], gats.at[pl.ds(0, 7)])
    arrived(ssem.at[2], toks.at[pl.ds(0, 7)])
    arrived(ssem.at[3], ys)
    arrived(ssem.at[4], part.at[pl.ds(0, 3)])


def solution(mesh):
    row_spec = P(('dp', 'ep2', 'ep'), None)
    weight_spec = P(('ep2', 'ep'), None, None)

    def local_step(tokens, expert_idx, gates, w_gate, w_up, w_down):
        rows, d_model = tokens.shape
        top_k = expert_idx.shape[1]
        n_exp, _, d_ff = w_gate.shape
        width = d_model // PIECES
        n_slot = n_exp * SLOT
        half = rows // 2
        hbm = pl.BlockSpec(memory_space=pl.ANY)
        n_sem = 22 + 5 * PIECES
        args = (tokens, expert_idx.T, gates.T, w_gate, w_up, w_down)
        args = [pltpu.with_memory_space_constraint(a, pltpu.HBM) for a in args]
        return pl.pallas_call(
            moe_kernel,
            out_shape=jax.ShapeDtypeStruct((rows, d_model), BF16),
            in_specs=[hbm] * 6,
            out_specs=pl.BlockSpec(memory_space=pltpu.VMEM),
            scratch_shapes=[
                pltpu.VMEM((n_exp, d_model, d_ff), BF16),
                pltpu.VMEM((n_exp, d_model, d_ff), BF16),
                pltpu.VMEM((n_exp, d_ff, d_model), BF16),
                pltpu.VMEM((8, rows, d_model), BF16),
                pltpu.VMEM((8, top_k, rows), jnp.int32),
                pltpu.VMEM((8, top_k, rows), F32),
                pltpu.VMEM((len(UNITS), 2, n_slot, rows), BF16),
                pltpu.VMEM((len(UNITS), 3, rows, 2 * n_slot), BF16),
                pltpu.VMEM((n_exp, 4 * SLOT, d_model), BF16),
                pltpu.VMEM((n_exp, 4 * SLOT, d_ff), BF16),
                pltpu.VMEM((len(UNITS), PIECES, 2 * n_slot, width), BF16),
                pltpu.VMEM((len(UNITS), PIECES, n_slot, width), BF16),
                pltpu.VMEM((4, 2 * PIECES, half, width), F32),
                pltpu.VMEM((2, PIECES, half, width), F32),
                pltpu.VMEM((2, PIECES, half, width), F32),
                pltpu.VMEM((2, PIECES, half, width), F32),
                pltpu.SemaphoreType.DMA((6,)),
                pltpu.SemaphoreType.DMA((5,)),
                pltpu.SemaphoreType.DMA((n_sem,)),
            ],
            compiler_params=pltpu.CompilerParams(
                collective_id=0, has_side_effects=True, vmem_limit_bytes=50 * 1024 * 1024
            ),
            name="moe",
        )(*args)

    return jax.shard_map(
        local_step, mesh=mesh,
        in_specs=(row_spec, row_spec, row_spec, weight_spec, weight_spec, weight_spec),
        out_specs=row_spec, check_vma=False,
    )
```

```python
import itertools

import jax
import jax.numpy as jnp
from jax import lax
from jax.experimental import pallas as pl
from jax.experimental.pallas import tpu as pltpu
from jax.sharding import PartitionSpec as P

MESH = pl.DeviceIdType.MESH
F32 = jnp.float32
BF16 = jnp.bfloat16
OWN, XN, YN, DG = 0, 1, 2, 3
SLOT = 32
UNITS = ((XN, 0, 64), (YN, 64, 64), (DG, 0, 128), (OWN, 0, 128), (XN, 64, 64), (YN, 0, 64))
EARLY = 32
LEAD = 16
PIECES = 3
BF16_MAX = float(jnp.finfo(jnp.bfloat16).max)


def moe_kernel(
    tok_hbm, idx_hbm, gate_hbm, wg_hbm, wu_hbm, wd_hbm, out_ref,
    wg, wu, wd, toks, idxs, gats, pick, mix, xg, hid, yc, ys, part, relb, finx, finy,
    lsem, ssem, rsem,
):
    n_exp = wg.shape[0]
    rows, d_model = out_ref.shape
    half = rows // 2
    width = d_model // PIECES
    n_slot = n_exp * SLOT
    top_k = idx_hbm.shape[0]

    def at(chip, core):
        return chip * 2 + core

    me = at(OWN, 0)
    own = [
        pltpu.make_async_copy(idx_hbm, idxs.at[me], lsem.at[0]),
        pltpu.make_async_copy(gate_hbm, gats.at[me], lsem.at[1]),
        pltpu.make_async_copy(tok_hbm, toks.at[me], lsem.at[2]),
    ]
    for copy in own:
        copy.start()
    loads = [
        pltpu.make_async_copy(src, dst, lsem.at[3 + i])
        for i, (src, dst) in enumerate(((wg_hbm, wg), (wu_hbm, wu), (wd_hbm, wd)))
    ]

    iy = lax.axis_index("ep2")
    ie = lax.axis_index("ep")
    ix = ie // 2
    ic = ie % 2
    to_x = {"ep2": iy, "ep": (1 - ix) * 2 + ic}
    to_y = {"ep2": 1 - iy, "ep": ie}
    to_c = {"ep2": iy, "ep": ix * 2 + 1 - ic}
    base_own = (iy * 4 + ie) * n_exp
    base_par = (iy * 4 + ix * 2 + 1 - ic) * n_exp

    barrier = pltpu.get_barrier_semaphore()
    for peer in (to_x, to_y, to_c):
        pl.semaphore_signal(barrier, inc=1, device_id=peer, device_id_type=MESH)
    for copy in loads:
        copy.start()
    pl.semaphore_wait(barrier, 3)

    ids = itertools.count()

    def new_sem():
        return rsem.at[next(ids)]

    def send(src, dst, peer, kind, sem):
        pltpu.make_async_remote_copy(
            src_ref=src, dst_ref=dst, send_sem=ssem.at[kind], recv_sem=sem,
            device_id=peer, device_id_type=MESH,
        ).start()

    def arrived(sem, like):
        pltpu.make_async_copy(like, like, sem).wait()

    def send_route(src, dst, peer):
        sem = new_sem()
        send(idx_hbm if src is None else idxs.at[src], idxs.at[dst], peer, 0, sem)
        send(gate_hbm if src is None else gats.at[src], gats.at[dst], peer, 1, sem)
        return lambda: arrived(sem, gats.at[pl.ds(0, 2)])

    def start_rows(src, dst, first, count, peer, sem):
        span = pl.ds(first, count)
        send((tok_hbm if src is None else toks.at[src]).at[span], toks.at[dst].at[span], peer, 2, sem)

    def send_rows(src, dst, first, peer, count=half):
        sem = new_sem()
        start_rows(src, dst, first, count, peer, sem)
        return lambda: arrived(sem, toks.at[dst].at[pl.ds(first, count)])

    r_x = send_route(None, at(XN, 0), to_x)
    r_y = send_route(None, at(YN, 0), to_y)
    t_x0 = send_rows(None, at(XN, 0), 0, to_x)
    t_y1 = send_rows(None, at(YN, 0), half, to_y)
    r_c = send_route(None, at(OWN, 1), to_c)
    for copy in own:
        copy.wait()

    sub16 = lax.broadcasted_iota(jnp.int32, (16, rows), 0)
    exp_id = jnp.where(sub16 < 8, base_own + sub16, base_par + sub16 - 8)
    row_i = lax.broadcasted_iota(jnp.int32, (rows, rows), 0)
    col_i = lax.broadcasted_iota(jnp.int32, (rows, rows), 1)
    before = jnp.where(row_i < col_i, 1.0, 0.0).astype(BF16)
    before_half = jnp.where((row_i < col_i) & ((row_i < half) == (col_i < half)), 1.0, 0.0).astype(BF16)
    place = lax.broadcasted_iota(jnp.int32, (SLOT, rows), 0).astype(F32)

    def prepare(chip, core):
        idx, gat = idxs[at(chip, core)], gats[at(chip, core)]
        chosen = jnp.zeros((16, rows), F32)
        weight = jnp.zeros((16, rows), F32)
        for j in range(top_k):
            hit = jnp.broadcast_to(idx[j:j + 1, :], (16, rows)) == exp_id
            chosen = jnp.where(hit, 1.0, chosen)
            weight = jnp.where(hit, jnp.broadcast_to(gat[j:j + 1, :], (16, rows)), weight)
        units = [(u, first, count) for u, (c, first, count) in enumerate(UNITS) if c == chip]
        order = before if len(units) == 1 else before_half
        rank = jnp.dot(chosen.astype(BF16), order, preferred_element_type=F32)
        rank = jnp.where(chosen > 0.0, rank, -1.0)
        for u, first, count in units:
            unit_rank = rank[:, first:first + count]
            for e in range(n_exp):
                here = jnp.broadcast_to(unit_rank[e:e + 1, :], (SLOT, count)) == place[:, :count]
                pick[u, core, pl.ds(e * SLOT, SLOT), pl.ds(0, count)] = jnp.where(here, 1.0, 0.0).astype(BF16)
        if core == 0:
            cols = []
            for k in range(2 * n_exp):
                row = k if k < n_exp else 8 + k - n_exp
                here = jnp.broadcast_to(rank[row:row + 1, :], (SLOT, rows)) == place
                cols.append(jnp.where(here, jnp.broadcast_to(weight[row:row + 1, :], (SLOT, rows)), 0.0))
            full = jnp.concatenate(cols, axis=0).T
            terms = [jnp.minimum(full, BF16_MAX).astype(BF16)]
            rest = full - terms[0].astype(F32)
            terms.append(rest.astype(BF16))
            terms.append((rest - terms[1].astype(F32)).astype(BF16))
            for u, first, count in units:
                for t in range(3):
                    mix[u, t, pl.ds(0, count), :] = terms[t][first:first + count, :]

    def gather(k, u, core):
        chip, first, count = UNITS[u]
        for n in range(PIECES):
            cols = pl.ds(n * width, width)
            got = jnp.dot(
                pick[u, core, :, pl.ds(0, count)], toks[at(chip, core), pl.ds(first, count), cols],
                preferred_element_type=F32,
            ).astype(BF16)
            for e in range(n_exp):
                xg[e, pl.ds(k * SLOT, SLOT), cols] = got[e * SLOT:(e + 1) * SLOT, :]

    def up_gate():
        for e in range(n_exp):
            a = jnp.dot(xg[e], wg[e], preferred_element_type=F32)
            b = jnp.dot(xg[e], wu[e], preferred_element_type=F32)
            hid[e] = (jax.nn.silu(a) * b).astype(BF16)

    def down(group, n, sems):
        for e in range(n_exp):
            y = jnp.dot(hid[e], wd[e, :, pl.ds(n * width, width)], preferred_element_type=F32).astype(BF16)
            for k, (u, core) in enumerate(group):
                dst = ys if core else yc
                dst[u, n, pl.ds(e * SLOT, SLOT), :] = y[k * SLOT:(k + 1) * SLOT, :]
        for u, core in group:
            if core:
                send(ys.at[u, n], yc.at[u, n].at[pl.ds(n_slot, n_slot)], to_c, 3, sems[u])

    def combine(u, n):
        chip, first, count = UNITS[u]
        y = yc[u, n]
        total = jnp.dot(mix[u, 2, pl.ds(0, count)], y, preferred_element_type=F32)
        total += jnp.dot(mix[u, 1, pl.ds(0, count)], y, preferred_element_type=F32)
        total += jnp.dot(mix[u, 0, pl.ds(0, count)], y, preferred_element_type=F32)
        for s in (0, 1):
            if first <= s * half < first + count:
                part[chip, s * PIECES + n] = total[s * half - first:(s + 1) * half - first, :]

    def send_sum(chip, s, n, sem, first=0, count=half):
        dst, peer = (finx, to_x) if chip == XN else (finy, to_y)
        span = pl.ds(first, count)
        send(part.at[chip, s * PIECES + n].at[span], dst.at[s, n].at[span], peer, 4, sem)

    r_x()
    r_xc = send_route(at(XN, 0), at(XN, 1), to_c)
    d_sem = new_sem()
    send(idxs.at[at(XN, 0)], idxs.at[at(DG, 0)], to_y, 0, d_sem)
    r_y()
    send(gats.at[at(YN, 0)], gats.at[at(DG, 0)], to_x, 1, d_sem)
    r_yc = send_route(at(YN, 0), at(YN, 1), to_c)
    prepare(XN, 0)
    prepare(YN, 0)
    r_xc()
    prepare(XN, 1)
    sem_x1, sem_y0 = new_sem(), new_sem()
    start_rows(me, at(XN, 0), half, EARLY, to_x, sem_x1)
    start_rows(me, at(YN, 0), 0, EARLY, to_y, sem_y0)
    r_yc()
    prepare(YN, 1)
    prepare(OWN, 0)
    r_c()
    prepare(OWN, 1)

    t_x0()
    t_d0 = send_rows(at(XN, 0), at(DG, 0), 0, to_y)
    t_xc0 = send_rows(at(XN, 0), at(XN, 1), 0, to_c)
    t_y1()
    t_d1 = send_rows(at(YN, 0), at(DG, 0), half, to_x)
    t_yc1 = send_rows(at(YN, 0), at(YN, 1), half, to_c)
    start_rows(me, at(XN, 0), half + EARLY, half - EARLY, to_x, sem_x1)
    start_rows(me, at(YN, 0), EARLY, half - EARLY, to_y, sem_y0)
    arrived(d_sem, gats.at[pl.ds(0, 2)])
    r_dc = send_route(at(DG, 0), at(DG, 1), to_c)
    t_c = send_rows(me, at(OWN, 1), 0, to_c, rows)

    group = ((0, 0), (0, 1), (1, 0), (1, 1))
    gather(0, *group[0])
    gather(2, *group[2])
    prepare(DG, 0)
    t_xc0()
    gather(1, *group[1])
    t_yc1()
    gather(3, *group[3])
    loads[0].wait()
    loads[1].wait()
    up_gate()
    loads[2].wait()
    sems = [new_sem() for _ in range(PIECES)]
    fin_first = new_sem()
    for n in range(PIECES):
        down(group, n, {0: sems[n], 1: sems[n]})
    for n in range(PIECES):
        arrived(sems[n], ys.at[pl.ds(0, 2), n])
        combine(0, n)
        send_sum(XN, 0, n, fin_first)
        combine(1, n)
        send_sum(YN, 1, n, fin_first)

    r_dc()
    prepare(DG, 1)
    group = ((2, 0), (2, 1), (3, 0), (3, 1))
    gather(2, *group[2])
    t_c()
    gather(3, *group[3])
    t_d0()
    t_dc0 = send_rows(at(DG, 0), at(DG, 1), 0, to_c)
    t_d1()
    t_dc1 = send_rows(at(DG, 0), at(DG, 1), half, to_c)
    gather(0, *group[0])
    t_dc0()
    t_dc1()
    gather(1, *group[1])
    up_gate()
    arrived(sem_x1, toks.at[at(XN, 0)].at[pl.ds(half, half)])
    t_xc1 = send_rows(at(XN, 0), at(XN, 1), half, to_c)
    arrived(sem_y0, toks.at[at(YN, 0)].at[pl.ds(0, half)])
    t_yc0 = send_rows(at(YN, 0), at(YN, 1), 0, to_c)
    sems = [new_sem() for _ in range(PIECES)]
    own_sem = new_sem()
    far = [new_sem() for _ in range(PIECES)]
    for n in range(PIECES):
        down(group, n, {2: sems[n], 3: own_sem})
    for n in range(PIECES):
        arrived(sems[n], ys.at[2, n])
        combine(2, n)
        send(part.at[DG, n], relb.at[0, n], to_x, 4, far[n])
        send(part.at[DG, PIECES + n], relb.at[1, n], to_y, 4, far[n])

    group = ((4, 0), (4, 1), (5, 0), (5, 1))
    t_xc1()
    t_yc0()
    for k in range(4):
        gather(k, *group[k])
    up_gate()
    rest_sem = new_sem()
    fin_last = [new_sem() for _ in range(PIECES)]
    for n in range(PIECES):
        down(group, n, {4: rest_sem, 5: rest_sem})
    arrived(rest_sem, ys.at[pl.ds(4, 2)])
    for n in range(PIECES):
        combine(4, n)
        combine(5, n)

    for n in range(PIECES):
        arrived(far[n], relb.at[:, n])
        part[YN, n] += relb[0, n]
        part[XN, PIECES + n] += relb[1, n]
        if n < PIECES - 1:
            send_sum(YN, 0, n, fin_last[n])
            send_sum(XN, 1, n, fin_last[n])
        else:
            send_sum(YN, 0, n, fin_last[n], 0, LEAD)
            send_sum(XN, 1, n, fin_last[n], 0, LEAD)
            pl.when(ic == 1)(lambda: arrived(fin_last[n - 1], finx.at[:, n - 1]))
            send_sum(YN, 0, n, fin_last[n], LEAD, half - LEAD)
            send_sum(XN, 1, n, fin_last[n], LEAD, half - LEAD)
        if n == 0:
            arrived(own_sem, ys.at[3])
            for m in range(PIECES):
                combine(3, m)
                for s in (0, 1):
                    part[OWN, s * PIECES + m] += toks[
                        me, pl.ds(s * half, half), pl.ds(m * width, width)
                    ].astype(F32)

    arrived(fin_first, finx)
    for n in range(PIECES):
        if n == PIECES - 2:
            pl.when(ic == 0)(lambda: arrived(fin_last[n], finx.at[:, n]))
        else:
            arrived(fin_last[n], finx.at[:, n])
        for s in (0, 1):
            out_ref[pl.ds(s * half, half), pl.ds(n * width, width)] = (
                part[OWN, s * PIECES + n] + finx[s, n] + finy[s, n]
            ).astype(BF16)
    arrived(ssem.at[0], idxs.at[pl.ds(0, 7)])
    arrived(ssem.at[1], gats.at[pl.ds(0, 7)])
    arrived(ssem.at[2], toks.at[pl.ds(0, 7)])
    arrived(ssem.at[3], ys)
    arrived(ssem.at[4], part.at[pl.ds(0, 3)])


def solution(mesh):
    row_spec = P(('dp', 'ep2', 'ep'), None)
    weight_spec = P(('ep2', 'ep'), None, None)

    def local_step(tokens, expert_idx, gates, w_gate, w_up, w_down):
        rows, d_model = tokens.shape
        top_k = expert_idx.shape[1]
        n_exp, _, d_ff = w_gate.shape
        width = d_model // PIECES
        n_slot = n_exp * SLOT
        half = rows // 2
        hbm = pl.BlockSpec(memory_space=pl.ANY)
        n_sem = 23 + 4 * PIECES
        args = (tokens, expert_idx.T, gates.T, w_gate, w_up, w_down)
        args = [pltpu.with_memory_space_constraint(a, pltpu.HBM) for a in args]
        return pl.pallas_call(
            moe_kernel,
            out_shape=jax.ShapeDtypeStruct((rows, d_model), BF16),
            in_specs=[hbm] * 6,
            out_specs=pl.BlockSpec(memory_space=pltpu.VMEM),
            scratch_shapes=[
                pltpu.VMEM((n_exp, d_model, d_ff), BF16),
                pltpu.VMEM((n_exp, d_model, d_ff), BF16),
                pltpu.VMEM((n_exp, d_ff, d_model), BF16),
                pltpu.VMEM((8, rows, d_model), BF16),
                pltpu.VMEM((8, top_k, rows), jnp.int32),
                pltpu.VMEM((8, top_k, rows), F32),
                pltpu.VMEM((len(UNITS), 2, n_slot, rows), BF16),
                pltpu.VMEM((len(UNITS), 3, rows, 2 * n_slot), BF16),
                pltpu.VMEM((n_exp, 4 * SLOT, d_model), BF16),
                pltpu.VMEM((n_exp, 4 * SLOT, d_ff), BF16),
                pltpu.VMEM((len(UNITS), PIECES, 2 * n_slot, width), BF16),
                pltpu.VMEM((len(UNITS), PIECES, n_slot, width), BF16),
                pltpu.VMEM((4, 2 * PIECES, half, width), F32),
                pltpu.VMEM((2, PIECES, half, width), F32),
                pltpu.VMEM((2, PIECES, half, width), F32),
                pltpu.VMEM((2, PIECES, half, width), F32),
                pltpu.SemaphoreType.DMA((6,)),
                pltpu.SemaphoreType.DMA((5,)),
                pltpu.SemaphoreType.DMA((n_sem,)),
            ],
            compiler_params=pltpu.CompilerParams(
                collective_id=0, has_side_effects=True, vmem_limit_bytes=50 * 1024 * 1024
            ),
            name="moe",
        )(*args)

    return jax.shard_map(
        local_step, mesh=mesh,
        in_specs=(row_spec, row_spec, row_spec, weight_spec, weight_spec, weight_spec),
        out_specs=row_spec, check_vma=False,
    )
```
